32 devices in a mesh: grp: 4 (over z), col: 8 (over y, x, core).
Axes of the slice: x: 2, y: 2, z: 4, core: 2. Of those that a mesh axis runs over, the one named last changes fastest.
Arguments:
- x_blocks: bfloat16 [16, 8, 6, 256, 256], P('grp', 'col'), may hold values from -6 to 6
- columns: int32 [16, 8, 6], replicated, may hold values from -1 to 127, as said below
- filter_ids: int32 [16, 8, 6], replicated, may hold values from 0 to 127, as said below
Outputs:
- sign_step: bfloat16 [16, 8, 6, 256, 256], P('grp', 'col')
The draws below stay inside these ranges and needn't reach their ends.
Inputs may be any that keep to these rules, and one draw needn't show every extreme that they name: `columns`: in each block row of the grid, slot 0 holds the row's own id; the other used slots hold distinct ids of block rows at most one step away along each grid dimension, with periodic wrap; used slots come first, then -1; at least 3 slots are used. `filter_ids`: in each block row, slot 0 holds the row's own id and the others distinct ids of block rows at most one step away along each grid dimension, with periodic wrap.
All inputs are finite; a program needn't handle non-finite values.
Results may differ from the reference program's by a relative error of at most 0.0019.
Values may be sent and summed in bfloat16 or wider, within the bound.
A program may use at most 128 MiB of HBM per device.

```python
import jax
import jax.numpy as jnp
from jax import lax

B = 256
KB = 6
KF = 6
NA = 16
NBC = 8


def neighbour_ids(key, slots):
    total_rows = NA * NBC
    row_keys = jax.random.split(key, total_rows)
    shuffled = jax.vmap(lambda one_key: jax.random.permutation(one_key, 8))(row_keys)
    others = shuffled + (shuffled >= 4).astype(shuffled.dtype)
    offset_code = jnp.concatenate([jnp.full((total_rows, 1), 4, jnp.int32), others.astype(jnp.int32)], axis=1)[:, :slots]
    step_a = offset_code // 3 - 1
    step_c = offset_code % 3 - 1
    row_index = jnp.arange(total_rows, dtype=jnp.int32)
    home_a = row_index // NBC
    home_c = row_index % NBC
    block_ids = (home_a[:, None] + step_a) % NA * NBC + (home_c[:, None] + step_c) % NBC
    return block_ids.astype(jnp.int32)


def draw_columns(key, part):
    total_rows = NA * NBC
    block_ids = neighbour_ids(jax.random.fold_in(key, 11), KB)
    counts = jax.random.randint(jax.random.fold_in(key, 12), (total_rows, 1), 3, KB + 1)
    slot_index = jnp.arange(KB, dtype=jnp.int32)[None, :]
    block_ids = jnp.where(slot_index < counts, block_ids, -1)
    return block_ids.reshape(NA, NBC, KB).astype(jnp.int32)


def draw_filter_ids(key, part):
    block_ids = neighbour_ids(jax.random.fold_in(key, 21), KF)
    return block_ids.reshape(NA, NBC, KF).astype(jnp.int32)


def level_of(stream_key, shape, pieces, low, top_value):
    gain = 1.0
    for axis_at, blocks in pieces:
        draws = jax.random.uniform(jax.random.fold_in(jax.random.fold_in(stream_key, 6), axis_at), (blocks,), jnp.float32, low / len(pieces), top_value / len(pieces))
        gain = gain * jnp.repeat(jnp.exp(draws), shape[axis_at] // blocks).reshape((-1,) + (1,) * (len(shape) - 1 - axis_at))
    return gain


def bell_draw(key, shape, scale, most, cuts=(), kind=jnp.bfloat16):
    loudness = level_of(key, shape, cuts, -0.22, 0.18) if cuts else 1.0
    values = jax.random.normal(key, shape, jnp.float32) * scale * loudness
    return jnp.minimum(jnp.maximum(values, -most), most).astype(kind)


def setup_inputs(seed: int = 0) -> dict:
    key_of = jax.random.split(jax.random.key(seed), 4)
    return {
        "x_blocks": bell_draw(key_of[0], (NA, NBC, KB, B, B), 1.0, 6.0, ((0, 4), (1, 8))),
        "columns": draw_columns(jax.random.fold_in(key_of[3], 71), 0),
        "filter_ids": draw_filter_ids(jax.random.fold_in(key_of[3], 71), 0),
    }


def locate(stored, wanted):
    matches = stored[:, None, :] == wanted[None, :, None]
    present = jnp.any(matches, axis=2) & (wanted[None, :] >= 0)
    slot_of = jnp.argmax(matches.astype(jnp.int32), axis=2).astype(jnp.int32)
    return slot_of, present


def reference(x_blocks, columns, filter_ids):
    total_rows = NA * NBC
    blocks = x_blocks.reshape(total_rows, KB, B, B)
    col_table = columns.reshape(total_rows, KB)
    filt_table = filter_ids.reshape(total_rows, KF)

    def square_row(row_index):
        row_cols = col_table[row_index]
        in_use = row_cols >= 0
        source = jnp.where(in_use, row_cols, 0)
        slot_of, present = locate(col_table[source], filt_table[row_index])
        present = present & in_use[:, None]
        picked = blocks[source[:, None], slot_of].astype(jnp.float32) * present[:, :, None, None].astype(jnp.float32)
        own = blocks[row_index].astype(jnp.float32)
        return jnp.einsum("kab,kfbc->fac", own, picked).astype(jnp.bfloat16)

    square = lax.map(square_row, jnp.arange(total_rows, dtype=jnp.int32))

    def sign_row(row_index):
        row_cols = col_table[row_index]
        in_use = row_cols >= 0
        source = jnp.where(in_use, row_cols, 0)
        slot_of, present = locate(filt_table[source], row_cols)
        present = present & in_use[:, None]
        picked = square[source[:, None], slot_of].astype(jnp.float32) * present[:, :, None, None].astype(jnp.float32)
        own = blocks[row_index].astype(jnp.float32)
        cubed = jnp.einsum("kab,kjbc->jac", own, picked)
        result = (1.5 * own - cubed * (0.5 / (KB * B))) * in_use[:, None, None].astype(jnp.float32)
        return result.astype(jnp.bfloat16)

    updated = lax.map(sign_row, jnp.arange(total_rows, dtype=jnp.int32))
    return updated.reshape(NA, NBC, KB, B, B)
```

```python
import functools

import jax
import jax.numpy as jnp
from jax import lax
from jax.experimental import pallas as pl
from jax.experimental.pallas import tpu as pltpu
from jax.sharding import PartitionSpec as P

MESH = pl.DeviceIdType.MESH
STEPS = [(da, dc) for da in (-1, 0, 1) for dc in (-1, 0, 1)]
FIRST = 3
CHUNK = 4
PACK = 128
STAIRS = (
    (14, 21, 19, 27, 5),
    (15, 22, 20, 28, 5),
    (16, 23, 21, 29, 5),
    (17, 24, 22, 30, 5),
    (18, 26, 23, 32, 5),
    (20, 29, 26, 36, 6),
)
LIMIT = 63 * 1024 * 1024


def grid_maps(shape, grid_a, grid_c, rows):
    rid = lax.broadcasted_iota(jnp.int32, shape, 1)
    a = jnp.zeros_like(rid)
    for i in range(1, grid_a):
        a = a + (rid >= i * grid_c).astype(jnp.int32)
    group = jnp.zeros_like(rid)
    for i in range(1, grid_a // rows):
        group = group + (a >= i * rows).astype(jnp.int32)
    return rid, rid - a * grid_c, a - group * rows, group


def row_of(x, i):
    return jnp.broadcast_to(x[i : i + 1], x.shape)


def most_of(x):
    return jnp.broadcast_to(jnp.max(x, axis=0, keepdims=True), x.shape)


def sum_of(x):
    return jnp.broadcast_to(jnp.sum(x, axis=0, keepdims=True), x.shape)


def layout(rows, slots):
    most = 3 * rows * slots
    bases = {"terms": 0, "pool": 88}
    bases["up"] = 88 + (most + 7) // 8 * 8
    bases["down"] = bases["up"] + 8
    bases["used"] = bases["up"] + 16
    bases["rows"] = bases["up"] + 24
    return bases


def plan_kernel(dims, cols_ref, filt_ref, tab1, tab2, level, laid, lists):
    rows, grid_a, grid_c, slots, levels = dims
    count = grid_a * grid_c
    held = rows * slots

    def roll(x, s, axis):
        s = s % x.shape[axis]
        return pltpu.roll(x, s, axis) if s else x

    def turned(ref):
        laid[...] = jnp.full(laid.shape, -1, jnp.int32)
        laid[:, :slots] = ref[...].reshape(count, slots)
        return laid[...].T[:8]

    cols, filt = turned(cols_ref), turned(filt_ref)
    rid, col, al, group = grid_maps(cols.shape, grid_a, grid_c, rows)
    sub = lax.broadcasted_iota(jnp.int32, cols.shape, 0)
    odd = lax.rem(col, 2) == 1
    quad = lax.rem(col, 4)
    facing = (quad == 1) | (quad == 2)
    low, high = al == 0, al == rows - 1

    def sh(x, step):
        da, dc = step
        x = roll(x, -da * grid_c, 1)
        if dc == 1:
            x = jnp.where(col == grid_c - 1, roll(x, grid_c - 1, 1), roll(x, -1, 1))
        if dc == -1:
            x = jnp.where(col == 0, roll(x, 1 - grid_c, 1), roll(x, 1, 1))
        return x

    def partner(x):
        return jnp.where(odd, roll(x, 1, 1), roll(x, -1, 1))

    def ahead_of(n):
        ahead = jnp.zeros_like(n)
        for s in range(1, slots):
            ahead = ahead + jnp.where(sub >= s, roll(n, s, 0), 0)
        return ahead

    def ranked(n):
        total = sum_of(n)
        before, after = jnp.zeros_like(n), jnp.zeros_like(n)
        for s in range(1, rows):
            before = before + jnp.where(al >= s, roll(total, s * grid_c, 1), 0)
            after = after + jnp.where(al < rows - s, roll(total, -s * grid_c, 1), 0)
        return before + ahead_of(n), before + total + after

    uses, kslot = [], []
    for step in STEPS:
        hit = (cols == sh(rid, step)).astype(jnp.int32)
        uses.append(most_of(hit))
        kslot.append(al * slots + sum_of(hit * sub))

    def needs(stored, wanted):
        asked = jnp.where(wanted < 0, -2, wanted)
        need = {(gd, dc): jnp.zeros_like(stored) for gd in (-1, 0, 1) for dc in (-1, 0, 1)}
        for i, (da, dc) in enumerate(STEPS):
            back = (-da, -dc)
            there = sh(asked, back)
            hit = jnp.zeros_like(stored)
            for f in range(slots):
                hit = hit | (stored == row_of(there, f)).astype(jnp.int32)
            hit = hit & sh(uses[i], back)
            at = al - da
            if dc:
                inside = ((at >= 0) & (at < rows)).astype(jnp.int32)
                need[0, -dc] = need[0, -dc] | (hit & inside)
            if da == -1:
                need[1, -dc] = need[1, -dc] | (hit & high.astype(jnp.int32))
            if da == 1:
                need[-1, -dc] = need[-1, -dc] | (hit & low.astype(jnp.int32))
        flat = jnp.where(odd, need[0, 1], need[0, -1])
        ups = need[1, 0] | need[1, 1] | need[1, -1]
        downs = need[-1, 0] | need[-1, 1] | need[-1, -1]
        corner = roll(jnp.where(odd, need[1, 1], need[1, -1]), grid_c, 1)
        corner = corner | roll(jnp.where(odd, need[-1, 1], need[-1, -1]), -grid_c, 1)
        rank, n = ranked(flat)
        crank, cn = ranked(corner)
        other, cother = partner(n), partner(cn)
        near = jnp.maximum(jnp.where(facing, n, other), FIRST)
        n_in = near + jnp.where(facing, other, n)
        n_corner = cn + cother
        rank = rank + jnp.where(facing, 0, near)
        crank = crank + jnp.where(facing, cother, 0)
        z_most = jnp.maximum(jnp.max(sum_of(ups)), jnp.max(sum_of(downs)))
        return asked, flat, rank, corner, crank, n_in, n_corner, ups, downs, z_most

    first = needs(cols, filt)
    second = needs(filt, cols)
    pick, failed = jnp.int32(0), jnp.int32(1)
    before = [jnp.int32(levels[0][0]), jnp.int32(levels[0][2])]
    for i, step in enumerate(levels[:-1]):
        over = (first[9] > step[4]) | (second[9] > step[4])
        for data, at, most in ((first, step[0], step[1]), (second, step[2], step[3])):
            over = over | (jnp.max(jnp.maximum(data[5], at) + data[6]) > most)
        failed = failed * over.astype(jnp.int32)
        pick = pick + failed
        for j in range(2):
            before[j] = jnp.where(failed > 0, levels[i + 1][2 * j], before[j])
    level[0] = pick

    grp, me = lax.axis_index("grp"), lax.axis_index("col")
    start = grp * rows * grid_c + me
    chip = (group == grp) & ((col - lax.rem(col, 2)) == (me - lax.rem(me, 2)))
    mine = (group == grp) & (col == me)
    absent = jnp.full_like(al, 2 * held * PACK)
    lay = layout(rows, slots)
    n_list = lay["up"] - lay["pool"]

    def here(x):
        return pltpu.roll(x, count - start, 1)[:, :128]

    def write(tab, stored, data, at):
        wanted, flat, rank, corner, crank, n_in, _, ups, downs, _ = data
        crank = crank + jnp.maximum(n_in, at)
        zup, zdown = ahead_of(ups), ahead_of(downs)
        zpos = jnp.where(low, roll(zup, grid_c, 1), slots + roll(zdown, -grid_c, 1))
        own = al * slots + sub
        codes = {}
        for i, (da, dc) in enumerate(STEPS):
            to = al + da
            inside = (to >= 0) & (to < rows)
            flat_at = sh(own, (da, dc))
            z_at = sh(zpos, (0, dc))
            if dc:
                outer = odd if dc == 1 else ~odd
                flat_at = jnp.where(outer, sh(rank, (da, dc)), held + flat_at)
                z_at = jnp.where(outer, sh(crank, (0, dc)), 2 * slots + z_at)
            place = jnp.where(inside, flat_at, z_at)
            kept = sh(stored, (da, dc))
            found = jnp.full_like(own, -1)
            for m in range(slots):
                found = jnp.where(wanted == row_of(kept, m), row_of(place, m), found)
            ok = (found >= 0) & (uses[i] > 0)
            codes[da, dc] = jnp.where(ok, kslot[i] * PACK + found, absent)
        for da in (-1, 0, 1):
            to = al + da
            inside = (to >= 0) & (to < rows)
            near = jnp.where(odd, codes[da, -1], codes[da, 1])
            far = jnp.where(odd, codes[da, 1], codes[da, -1])
            for j, x in ((0, codes[da, 0]), (1, near)):
                at_row = (j * 3 + da + 1) * 8
                tab[at_row : at_row + 8, :] = here(jnp.where(inside, x, absent))
            at_row = (8 + da + 1) * 8
            tab[at_row : at_row + 8, :] = here(far)
        for j in range(2):
            pair = []
            for da in (-1, 1):
                near = jnp.where(odd, codes[da, -1], codes[da, 1])
                pair.append(codes[da, 0] if j == 0 else near)
            z = jnp.where(low, pair[0], jnp.where(high, pair[1], absent))
            tab[(6 + j) * 8 : (7 + j) * 8, :] = here(z)
        side = jnp.where(col == me, 0, 1)
        flat_code = jnp.where(chip & (flat > 0), own + side * held + 1, 0)
        corner_code = jnp.where(chip & (corner > 0), PACK + zpos + side * 2 * slots + 1, 0)
        for j in range(n_list):
            x = jnp.where(rank == j, flat_code, 0)
            x = jnp.maximum(x, jnp.where(crank == j, corner_code, 0))
            lists[j : j + 1, :] = jnp.max(x, axis=0, keepdims=True)
        up_code = jnp.where(mine & (ups > 0), own, 0)
        down_code = jnp.where(mine & (downs > 0), own, 0)
        for j in range(8):
            x = jnp.where(zup == j, up_code, 0)
            lists[n_list + j : n_list + j + 1, :] = jnp.max(x, axis=0, keepdims=True)
            x = jnp.where(zdown == j, down_code, 0)
            lists[n_list + 8 + j : n_list + 9 + j, :] = jnp.max(x, axis=0, keepdims=True)
        found = jnp.max(lists[...], axis=1, keepdims=True)
        tab[lay["pool"] : lay["used"], :] = jnp.broadcast_to(found, (n_list + 16, 128))
        tab[lay["used"] : lay["rows"], :] = here((cols >= 0).astype(jnp.int32))

    write(tab1, cols, first, before[0])
    write(tab2, filt, second, before[1])


def pieces(start, stop):
    out = []
    while start < stop:
        n = min(CHUNK, stop - start)
        out.append((start, n))
        start += n
    return out


def main_kernel(
    dims,
    sizes,
    scale,
    tab1,
    tab2,
    x,
    out,
    both1,
    both2,
    squares,
    zone1,
    zone2,
    outer1,
    outer2,
    pool,
    zsend,
    acc,
    dsend,
    drecv,
    zs_sem,
    zr_sem,
    zf_send,
    zf_recv,
    xs_sem,
    xr_sem,
    ys_sem,
):
    rows, grid_c, slots = dims
    held = rows * slots
    lay = layout(rows, slots)
    grp, col = lax.axis_index("grp"), lax.axis_index("col")
    grps = lax.axis_size("grp")
    quad = lax.rem(col, 4)
    odd = lax.rem(col, 2)
    facing = (quad == 1) | (quad == 2)
    sign = 1 - 2 * odd
    partner = (grp, col + sign)
    above = (lax.rem(grp + 1, grps), col)
    below = (lax.rem(grp + grps - 1, grps), col)
    across = (grp, lax.rem(col - sign + grid_c, grid_c))
    relay = (grp, lax.rem(col - 3 * sign + grid_c, grid_c))

    barrier = pltpu.get_barrier_semaphore()
    for peer in (partner, above, below, relay):
        pl.semaphore_signal(barrier, inc=1, device_id=peer, device_id_type=MESH)

    @pl.when(facing)
    def _():
        pl.semaphore_signal(barrier, inc=1, device_id=across, device_id_type=MESH)
        pl.semaphore_wait(barrier, 5)

    @pl.when(jnp.logical_not(facing))
    def _():
        pl.semaphore_wait(barrier, 4)

    def remote(src, dst, send_sem, recv_sem, peer):
        return pltpu.make_async_remote_copy(
            src_ref=src, dst_ref=dst, send_sem=send_sem, recv_sem=recv_sem, device_id=peer, device_id_type=MESH
        )

    def each(n, body):
        def one(i, carry):
            body(i)
            return carry

        lax.fori_loop(0, n, one, 0)

    def times(tab, row, lane, right):
        code = tab[row, lane]
        return jnp.dot(
            both1[lax.div(code, PACK)], right[lax.rem(code, PACK)], preferred_element_type=jnp.float32
        )

    def phase(at, tab, src, both, zone, outer, split, most, zn, finish):
        spread = remote(src, both.at[pl.ds(held, held)], dsend.at[at], drecv.at[at], partner)
        spread.start()

        def up(j):
            zsend[j] = src[tab[lay["up"] + j, 0]]

        def down(j):
            zsend[slots + j] = src[tab[lay["down"] + j, 0]]

        each(zn, up)
        each(zn, down)
        zcopies = [
            remote(zsend.at[pl.ds(s * slots, zn)], zone.at[pl.ds(s * slots, zn)], zs_sem.at[at, s], zr_sem.at[at, s], peer)
            for s, peer in ((0, above), (1, below))
        ]
        for copy in zcopies:
            copy.start()
        parts = [(0, FIRST)] + pieces(FIRST, split) + pieces(split, most)
        early = 1 + len(pieces(FIRST, split))
        xcopies, ycopies = [], []
        for i, (lo, n) in enumerate(parts):
            xcopies.append(
                remote(pool.at[pl.ds(lo, n)], outer.at[pl.ds(lo, n)], xs_sem.at[at, i], xr_sem.at[at, i], across)
            )
            ycopies.append(
                remote(outer.at[pl.ds(lo, n)], outer.at[pl.ds(lo, n)], ys_sem.at[at, i], xr_sem.at[at, i], relay)
            )

        @pl.when(facing)
        def _():
            def one(j):
                pool[j] = src[lax.max(tab[lay["pool"] + j, 0] - 1, 0)]

            each(FIRST, one)
            xcopies[0].start()

        if at == 0:

            def keep(i):
                both[i] = src[i]

            each(held, keep)
            both[2 * held] = jnp.zeros(both.shape[1:], both.dtype)
        spread.wait_recv()

        @pl.when(facing)
        def _():
            def one(j):
                pool[j] = both[lax.max(tab[lay["pool"] + j, 0] - 1, 0)]

            for i in range(1, early):
                lo, n = parts[i]
                each(n, lambda j, lo=lo: one(lo + j))
                xcopies[i].start()

        def inner(a, carry):
            def one(f, carry):
                total = None
                for j in range(6):
                    term = times(tab, j * 8 + f, a * grid_c, both)
                    total = term if total is None else total + term
                acc[a * slots + f] = total
                return carry

            return lax.fori_loop(0, slots, one, carry)

        lax.fori_loop(0, rows, inner, 0)

        @pl.when(facing)
        def _():
            for i in range(early - 1):
                xcopies[i].wait_recv()
                ycopies[i].start()

        zpass = []
        for s, copy in enumerate(zcopies):
            copy.wait_recv()
            onward = remote(
                zone.at[pl.ds(s * slots, zn)],
                zone.at[pl.ds((2 + s) * slots, zn)],
                zf_send.at[at, s],
                zf_recv.at[at, s],
                partner,
            )
            onward.start()
            zpass.append(onward)
        for copy in zpass:
            copy.wait_recv()

        @pl.when(facing)
        def _():
            def one(j):
                code = tab[lay["pool"] + j, 0]
                far = (code > PACK).astype(jnp.int32)
                a = both[lax.max(code - 1, 0) * (1 - far)].astype(jnp.float32)
                b = zone[(code - PACK - 1) * far].astype(jnp.float32)
                w = far.astype(jnp.float32)
                pool[j] = (a * (1.0 - w) + b * w).astype(pool.dtype)

            for i in range(early, len(parts)):
                lo, n = parts[i]
                each(n, lambda j, lo=lo: one(lo + j))
                xcopies[i].start()

        def edge(e, carry):
            a = e * (rows - 1)

            def one(f, carry):
                total = times(tab, 48 + f, a * grid_c, zone) + times(tab, 56 + f, a * grid_c, zone)
                acc[a * slots + f] += total
                return carry

            return lax.fori_loop(0, slots, one, carry)

        lax.fori_loop(0, 2, edge, 0)

        @pl.when(facing)
        def _():
            for i in range(early - 1, len(parts)):
                xcopies[i].wait_recv()
                ycopies[i].start()

        @pl.when(jnp.logical_not(facing))
        def _():
            for copy in ycopies:
                copy.wait_recv()

        def last(a, carry):
            def one(f, carry):
                total = acc[a * slots + f]
                for j in range(3):
                    total = total + times(tab, 64 + j * 8 + f, a * grid_c, outer)
                finish(a, f, total)
                return carry

            return lax.fori_loop(0, slots, one, carry)

        lax.fori_loop(0, rows, last, 0)
        spread.wait_send()
        for copy in zcopies + zpass:
            copy.wait_send()

        @pl.when(facing)
        def _():
            for copy in xcopies + ycopies:
                copy.wait_send()

    def square(a, f, total):
        value = total.astype(squares.dtype)
        squares[a * slots + f] = value
        both2[a * slots + f] = value

    def step(a, f, total):
        used = tab1[lay["used"] + f, a * grid_c].astype(jnp.float32)
        value = 1.5 * x[a * slots + f].astype(jnp.float32) - total * scale
        out[a * slots + f] = (value * used).astype(out.dtype)

    split1, most1, split2, most2, zn = sizes
    phase(0, tab1, x, both1, zone1, outer1, split1, most1, zn, square)
    phase(1, tab2, squares, both2, zone2, outer2, split2, most2, zn, step)


def local(x_blocks, columns, filter_ids):
    grps, ncol = lax.axis_size("grp"), lax.axis_size("col")
    rows, per_col, slots, order = x_blocks.shape[:4]
    assert per_col == 1 and filter_ids.shape[2] == slots and ncol % 4 == 0 and rows > 1
    grid_a, grid_c = rows * grps, ncol
    count = grid_a * grid_c
    held = rows * slots
    blocks = x_blocks.reshape(held, order, order)
    dtype = blocks.dtype
    full = (2 * held, 3 * held)
    levels = [s for s in STAIRS if s[1] < full[1] and s[3] < full[1]] + [full + full + (slots,)]
    lay = layout(rows, slots)
    vmem = pl.BlockSpec(memory_space=pltpu.VMEM)
    smem = pl.BlockSpec(memory_space=pltpu.SMEM)
    table = jax.ShapeDtypeStruct((lay["rows"], 128), jnp.int32)
    tab1, tab2, level = pl.pallas_call(
        functools.partial(plan_kernel, (rows, grid_a, grid_c, slots, levels)),
        out_shape=[table, table, jax.ShapeDtypeStruct((1,), jnp.int32)],
        in_specs=[vmem, vmem],
        out_specs=[vmem, vmem, smem],
        scratch_shapes=[
            pltpu.VMEM((count, 128), jnp.int32),
            pltpu.VMEM((lay["used"] - lay["pool"], count), jnp.int32),
        ],
        name="plan",
    )(columns, filter_ids)

    def blocks_of(n):
        return pltpu.VMEM((n, order, order), dtype)

    branches = []
    for i, sizes in enumerate(levels):
        split1, most1, split2, most2, zn = sizes
        parts = 1 + max(
            len(pieces(FIRST, split1)) + len(pieces(split1, most1)),
            len(pieces(FIRST, split2)) + len(pieces(split2, most2)),
        )
        dma = pltpu.SemaphoreType.DMA
        branches.append(
            pl.pallas_call(
                functools.partial(main_kernel, (rows, grid_c, slots), sizes, 0.5 / (slots * order)),
                out_shape=jax.ShapeDtypeStruct(blocks.shape, dtype),
                in_specs=[smem, smem, vmem],
                out_specs=vmem,
                scratch_shapes=[
                    blocks_of(2 * held + 1),
                    blocks_of(2 * held),
                    blocks_of(held),
                    blocks_of(4 * slots),
                    blocks_of(4 * slots),
                    blocks_of(most1),
                    blocks_of(most2),
                    blocks_of(max(most1, most2)),
                    blocks_of(2 * slots),
                    pltpu.VMEM((held, order, order), jnp.float32),
                    dma((2,)),
                    dma((2,)),
                    dma((2, 2)),
                    dma((2, 2)),
                    dma((2, 2)),
                    dma((2, 2)),
                    dma((2, parts)),
                    dma((2, parts)),
                    dma((2, parts)),
                ],
                compiler_params=pltpu.CompilerParams(
                    collective_id=i, has_side_effects=True, vmem_limit_bytes=LIMIT
                ),
                name="step_%d_%d" % (most1, most2),
            )
        )
    out = lax.switch(level[0], branches, tab1, tab2, blocks)
    return out.reshape(x_blocks.shape)


def solution(mesh):
    return jax.shard_map(
        local,
        mesh=mesh,
        in_specs=(P("grp", "col", None, None, None), P(), P()),
        out_specs=P("grp", "col", None, None, None),
        check_vma=False,
    )
```

```python
import functools

import jax
import jax.numpy as jnp
from jax import lax
from jax.experimental import pallas as pl
from jax.experimental.pallas import tpu as pltpu
from jax.sharding import PartitionSpec as P

MESH = pl.DeviceIdType.MESH
STEPS = [(da, dc) for da in (-1, 0, 1) for dc in (-1, 0, 1)]
FIRST = 3
ZFIRST = 2
PACK = 128
STAIRS = (
    (16, 22, 24, 8, 20, 26, 28, 9),
    (16, 22, 24, 8, 20, 26, 30, 9),
    (16, 22, 25, 8, 20, 26, 32, 10),
    (16, 22, 28, 10, 20, 26, 31, 10),
    (16, 22, 25, 8, 20, 26, 35, 12),
    (16, 22, 27, 10, 20, 26, 34, 10),
    (16, 22, 31, 10, 20, 26, 38, 12),
)
LIMIT = 63 * 1024 * 1024


def grid_maps(shape, grid_a, grid_c, rows):
    rid = lax.broadcasted_iota(jnp.int32, shape, 1)
    a = jnp.zeros_like(rid)
    for i in range(1, grid_a):
        a = a + (rid >= i * grid_c).astype(jnp.int32)
    group = jnp.zeros_like(rid)
    for i in range(1, grid_a // rows):
        group = group + (a >= i * rows).astype(jnp.int32)
    return rid, rid - a * grid_c, a - group * rows, group


def row_of(x, i):
    return jnp.broadcast_to(x[i : i + 1], x.shape)


def most_of(x):
    return jnp.broadcast_to(jnp.max(x, axis=0, keepdims=True), x.shape)


def sum_of(x):
    return jnp.broadcast_to(jnp.sum(x, axis=0, keepdims=True), x.shape)


def layout(rows, slots):
    bases = {"terms": 0, "used": 88, "up": 96}
    bases["down"] = 96 + 2 * slots
    bases["pool"] = 96 + 4 * slots
    bases["end"] = bases["pool"] + 3 * rows * slots
    bases["width"] = (bases["end"] + 127) // 128 * 128
    return bases


def plan_kernel(dims, cols_ref, filt_ref, tab1, tab2, level, lists, wide):
    rows, grid_a, grid_c, slots, levels = dims
    count = grid_a * grid_c
    held = rows * slots

    def roll(x, s, axis):
        s = s % x.shape[axis]
        return pltpu.roll(x, s, axis) if s else x

    shape = (8, count)
    rid, col, al, group = grid_maps(shape, grid_a, grid_c, rows)
    lane_row = lax.broadcasted_iota(jnp.int32, (grid_a, count), 1) // grid_c
    spread = (lane_row == lax.broadcasted_iota(jnp.int32, (grid_a, count), 0)).astype(jnp.float32)
    pick_col = lax.broadcasted_iota(jnp.int32, (grid_c, count), 1) % grid_c
    pick_col = pick_col == lax.broadcasted_iota(jnp.int32, (grid_c, count), 0)

    def laid(ref):
        flat = ref[...].reshape(slots * grid_c, grid_a).astype(jnp.float32)
        wide_ids = jnp.dot(flat, spread, precision=lax.Precision.HIGHEST, preferred_element_type=jnp.float32)
        sub = lax.broadcasted_iota(jnp.int32, shape, 0)
        ids = jnp.full(shape, -1, jnp.int32)
        for k in range(slots):
            part = jnp.where(pick_col, wide_ids[k * grid_c : (k + 1) * grid_c], 0.0)
            line = jnp.sum(part, axis=0, keepdims=True).astype(jnp.int32)
            ids = jnp.where(sub == k, jnp.broadcast_to(line, shape), ids)
        return ids

    cols, filt = laid(cols_ref), laid(filt_ref)
    sub = lax.broadcasted_iota(jnp.int32, cols.shape, 0)
    odd = lax.rem(col, 2) == 1
    quad = lax.rem(col, 4)
    facing = (quad == 1) | (quad == 2)
    low, high = al == 0, al == rows - 1

    def sh(x, step):
        da, dc = step
        x = roll(x, -da * grid_c, 1)
        if dc == 1:
            x = jnp.where(col == grid_c - 1, roll(x, grid_c - 1, 1), roll(x, -1, 1))
        if dc == -1:
            x = jnp.where(col == 0, roll(x, 1 - grid_c, 1), roll(x, 1, 1))
        return x

    def partner(x):
        return jnp.where(odd, roll(x, 1, 1), roll(x, -1, 1))

    def ahead_of(n):
        ahead = jnp.zeros_like(n)
        for s in range(1, slots):
            ahead = ahead + jnp.where(sub >= s, roll(n, s, 0), 0)
        return ahead

    def ranked(n):
        total = sum_of(n)
        before, after = jnp.zeros_like(n), jnp.zeros_like(n)
        for s in range(1, rows):
            before = before + jnp.where(al >= s, roll(total, s * grid_c, 1), 0)
            after = after + jnp.where(al < rows - s, roll(total, -s * grid_c, 1), 0)
        return before + ahead_of(n), before + total + after

    uses, kslot = [], []
    for step in STEPS:
        hit = (cols == sh(rid, step)).astype(jnp.int32)
        uses.append(most_of(hit))
        kslot.append(al * slots + sum_of(hit * sub))

    def needs(stored, wanted):
        asked = jnp.where(wanted < 0, -2, wanted)
        need = {(gd, dc): jnp.zeros_like(stored) for gd in (-1, 0, 1) for dc in (-1, 0, 1)}
        for i, (da, dc) in enumerate(STEPS):
            back = (-da, -dc)
            there = sh(asked, back)
            hit = jnp.zeros_like(stored)
            for f in range(slots):
                hit = hit | (stored == row_of(there, f)).astype(jnp.int32)
            hit = hit & sh(uses[i], back)
            at = al - da
            if dc:
                inside = ((at >= 0) & (at < rows)).astype(jnp.int32)
                need[0, -dc] = need[0, -dc] | (hit & inside)
            if da == -1:
                need[1, -dc] = need[1, -dc] | (hit & high.astype(jnp.int32))
            if da == 1:
                need[-1, -dc] = need[-1, -dc] | (hit & low.astype(jnp.int32))
        flat = jnp.where(odd, need[0, 1], need[0, -1])
        ups = need[1, 0] | need[1, 1] | need[1, -1]
        downs = need[-1, 0] | need[-1, 1] | need[-1, -1]
        corner = roll(jnp.where(odd, need[1, 1], need[1, -1]), grid_c, 1)
        corner = corner | roll(jnp.where(odd, need[-1, 1], need[-1, -1]), -grid_c, 1)
        rank, n = ranked(flat)
        crank, cn = ranked(corner)
        other, cother = partner(n), partner(cn)
        n_near, n_far = jnp.where(facing, n, other), jnp.where(facing, other, n)
        c_near, c_far = jnp.where(facing, cn, cother), jnp.where(facing, cother, cn)
        rank = rank + jnp.where(facing, jnp.where(rank >= FIRST, n_far, 0), FIRST)
        n_in = FIRST + n_far + jnp.maximum(n_near - FIRST, 0)
        zups, zdowns, zmost = [], [], []
        for lists_of, src in ((zups, ups), (zdowns, downs)):
            total = sum_of(src)
            base = jnp.where(facing, jnp.maximum(partner(total), ZFIRST), 0)
            lists_of.append(ahead_of(src) + base)
            zmost.append(jnp.max(base + total))
        z_most = jnp.maximum(zmost[0], zmost[1])
        return {
            "wanted": asked,
            "flat": flat,
            "rank": rank,
            "corner": corner,
            "crank": crank,
            "n_in": n_in,
            "n_far": n_far,
            "c_near": c_near,
            "c_far": c_far,
            "ups": ups,
            "downs": downs,
            "zup": zups[0],
            "zdown": zdowns[0],
            "z_most": z_most,
        }

    first = needs(cols, filt)
    second = needs(filt, cols)
    pick, failed = jnp.int32(0), jnp.int32(1)
    before = [jnp.int32(levels[0][0]), jnp.int32(levels[0][4])]
    for i, step in enumerate(levels[:-1]):
        over = jnp.bool_(False)
        for data, (at, reach, most, zn) in ((first, step[:4]), (second, step[4:])):
            total = jnp.maximum(data["n_in"], at) + data["c_near"] + data["c_far"]
            passed = jnp.maximum(data["n_far"] + FIRST, at) + data["c_far"]
            over = over | (jnp.max(total) > most) | (jnp.max(passed) > reach) | (data["z_most"] > zn)
        failed = failed * over.astype(jnp.int32)
        pick = pick + failed
        for j in range(2):
            before[j] = jnp.where(failed > 0, levels[i + 1][4 * j], before[j])
    level[0] = pick

    grp, me = lax.axis_index("grp"), lax.axis_index("col")
    start = grp * rows * grid_c + me
    chip = (group == grp) & ((col - lax.rem(col, 2)) == (me - lax.rem(me, 2)))
    absent = jnp.full_like(al, 2 * held * PACK)
    absent_far = absent + FIRST
    lay = layout(rows, slots)

    def here(x):
        return pltpu.roll(x, count - start, 1)[:, :128]

    def write(tab, stored, data, at):
        wanted = data["wanted"]
        rank = data["rank"] + jnp.where(data["rank"] >= at, data["c_far"], 0)
        crank = data["crank"] + jnp.where(facing, jnp.maximum(data["n_in"], at) + data["c_far"], at)
        zpos = jnp.where(low, roll(data["zup"], grid_c, 1), 2 * slots + roll(data["zdown"], -grid_c, 1))
        own = al * slots + sub
        codes = {}
        for i, (da, dc) in enumerate(STEPS):
            to = al + da
            inside = (to >= 0) & (to < rows)
            flat_at = sh(own, (da, dc))
            z_at = sh(zpos, (0, dc))
            none = absent
            if dc:
                outer = odd if dc == 1 else ~odd
                flat_at = jnp.where(outer, sh(rank, (da, dc)), held + flat_at)
                z_at = jnp.where(outer, sh(crank, (0, dc)), z_at)
                none = jnp.where(outer, absent_far, absent)
            place = jnp.where(inside, flat_at, z_at)
            kept = sh(stored, (da, dc))
            found = jnp.full_like(own, -1)
            for m in range(slots):
                found = jnp.where(wanted == row_of(kept, m), row_of(place, m), found)
            ok = (found >= 0) & (uses[i] > 0)
            codes[da, dc] = jnp.where(ok, kslot[i] * PACK + found, none)
        for da in (-1, 0, 1):
            to = al + da
            inside = (to >= 0) & (to < rows)
            near = jnp.where(odd, codes[da, -1], codes[da, 1])
            far = jnp.where(odd, codes[da, 1], codes[da, -1])
            for j, x in ((0, codes[da, 0]), (1, near)):
                at_row = (j * 3 + da + 1) * 8
                wide[at_row : at_row + 8, :] = here(jnp.where(inside, x, absent))
            at_row = (8 + da + 1) * 8
            wide[at_row : at_row + 8, :] = here(far)
        for j in range(2):
            pair = []
            for da in (-1, 1):
                near = jnp.where(odd, codes[da, -1], codes[da, 1])
                pair.append(codes[da, 0] if j == 0 else near)
            z = jnp.where(low, pair[0], jnp.where(high, pair[1], absent))
            wide[(6 + j) * 8 : (7 + j) * 8, :] = here(z)
        wide[lay["used"] : lay["used"] + 8, :] = here((cols >= 0).astype(jnp.int32))
        side = jnp.where(col == me, 0, 1)
        block = own + side * held + 1
        flat_code = jnp.where(chip & (data["flat"] > 0), block, 0)
        corner_code = jnp.where(chip & (data["corner"] > 0), PACK + zpos + 1, 0)
        up_code = jnp.where(chip & (data["ups"] > 0), block, 0)
        down_code = jnp.where(chip & (data["downs"] > 0), block, 0)
        base = lay["up"]

        def put(row, x):
            lists[row - base : row - base + 1, :] = jnp.max(x, axis=0, keepdims=True)

        for j in range(2 * slots):
            put(lay["up"] + j, jnp.where(data["zup"] == j, up_code, 0))
            put(lay["down"] + j, jnp.where(data["zdown"] == j, down_code, 0))
        for j in range(lay["end"] - lay["pool"]):
            x = jnp.where(rank == j, flat_code, 0)
            put(lay["pool"] + j, jnp.maximum(x, jnp.where(crank == j, corner_code, 0)))
        found = jnp.max(lists[...], axis=1, keepdims=True)
        wide[base : lay["end"], :] = jnp.broadcast_to(found, (lay["end"] - base, 128))
        turned = wide[...].T
        for a in range(rows):
            tab[a : a + 1, :] = turned[a * grid_c : a * grid_c + 1, :]

    write(tab1, cols, first, before[0])
    write(tab2, filt, second, before[1])


def pieces(start, stop, most):
    out = []
    while start < stop:
        n = min(most, stop - start)
        out.append((start, n))
        start += n
    return out


def cut(split, reach, most):
    out = [(0, FIRST)] + pieces(FIRST, split, 4) + pieces(split, reach, 2) + pieces(reach, most, 2)
    return out


def main_kernel(
    dims,
    sizes,
    scale,
    tab1,
    tab2,
    x,
    out,
    both1,
    both2,
    squares,
    zone1,
    zone2,
    outer1,
    outer2,
    pool,
    acc,
    dsend,
    drecv,
    zs_sem,
    zr_sem,
    zf_send,
    zf_recv,
    xs_sem,
    xr_sem,
    ys_sem,
):
    rows, grid_c, slots = dims
    held = rows * slots
    lay = layout(rows, slots)
    grp, col = lax.axis_index("grp"), lax.axis_index("col")
    grps = lax.axis_size("grp")
    quad = lax.rem(col, 4)
    odd = lax.rem(col, 2)
    facing = (quad == 1) | (quad == 2)
    sign = 1 - 2 * odd
    partner = (grp, col + sign)
    above = (lax.rem(grp + 1, grps), col)
    below = (lax.rem(grp + grps - 1, grps), col)
    across = (grp, lax.rem(col - sign + grid_c, grid_c))
    relay = (grp, lax.rem(col - 3 * sign + grid_c, grid_c))

    barrier = pltpu.get_barrier_semaphore()
    for peer in (partner, relay):
        pl.semaphore_signal(barrier, inc=1, device_id=peer, device_id_type=MESH)

    @pl.when(facing)
    def _():
        pl.semaphore_signal(barrier, inc=1, device_id=across, device_id_type=MESH)
        pl.semaphore_wait(barrier, 3)

    @pl.when(jnp.logical_not(facing))
    def _():
        for peer in (above, below):
            pl.semaphore_signal(barrier, inc=1, device_id=peer, device_id_type=MESH)
        pl.semaphore_wait(barrier, 4)

    def remote(src, dst, send_sem, recv_sem, peer):
        return pltpu.make_async_remote_copy(
            src_ref=src, dst_ref=dst, send_sem=send_sem, recv_sem=recv_sem, device_id=peer, device_id_type=MESH
        )

    def each(lo, hi, body):
        def one(i, carry):
            body(i)
            return carry

        lax.fori_loop(lo, hi, one, 0)

    def product(tab, row, a, right):
        code = tab[a, row]
        return jnp.dot(
            both1[lax.div(code, PACK)], right[lax.rem(code, PACK)], preferred_element_type=jnp.float32
        )

    def totals(tab, a, base, terms, wide, right, put):
        def one(i, carry):
            sums = [None] * wide
            for j in range(terms):
                for q in range(wide):
                    term = product(tab, base + j * 8 + i * wide + q, a, right)
                    sums[q] = term if sums[q] is None else sums[q] + term
            for q in range(wide):
                put(i * wide + q, sums[q])
            return carry

        lax.fori_loop(0, slots // wide, one, 0)

    def phase(at, tab, src, both, zone, outer, sizes, finish):
        split, reach, most, zn = sizes
        not_facing = jnp.logical_not(facing)
        spread = remote(src, both.at[pl.ds(held, held)], dsend.at[at], drecv.at[at], partner)
        spread.start()
        parts = cut(split, reach, most)
        xcopies, ycopies = [], []
        for i, (lo, n) in enumerate(parts):
            place = outer.at[pl.ds(lo, n)]
            xcopies.append(remote(pool.at[pl.ds(lo, n)], place, xs_sem.at[at, i], xr_sem.at[at, i], across))
            ycopies.append(remote(place, place, ys_sem.at[at, i], xr_sem.at[at, i], relay) if 0 < lo < reach else None)
        early = sum(lo < split for lo, _ in parts)
        passed = range(1, sum(lo < reach for lo, _ in parts))
        zcopies, zpass = [], []
        for s, peer in ((0, above), (1, below)):
            for i, (lo, n) in enumerate(((0, ZFIRST), (ZFIRST, zn - ZFIRST))):
                piece = pl.ds(2 * s * slots + lo, n)
                sems = zs_sem.at[at, s, i], zr_sem.at[at, s, i]
                zcopies.append(remote(pool.at[piece], zone.at[piece], *sems, peer))
            piece = pl.ds(2 * s * slots, zn)
            zpass.append(remote(zone.at[piece], zone.at[piece], zf_send.at[at, s], zf_recv.at[at, s], partner))

        def gather(dst, src, base, lo, n, to):
            def one(j):
                dst[to + j] = src[lax.max(tab[0, base + j] - 1, 0)]

            each(lo, lo + n, one)

        @pl.when(facing)
        def _():
            gather(pool, src, lay["pool"], 0, FIRST, 0)
            xcopies[0].start()

        @pl.when(not_facing)
        def _():
            for s, base in ((0, lay["up"]), (1, lay["down"])):
                gather(pool, src, base, 0, ZFIRST, 2 * s * slots)
                zcopies[2 * s].start()

        if at == 0:

            def keep(i):
                both[i] = src[i]

            each(0, held, keep)
            both[2 * held] = jnp.zeros(both.shape[1:], both.dtype)
        spread.wait_recv()

        @pl.when(facing)
        def _():
            for i in range(1, early):
                gather(pool, both, lay["pool"], *parts[i], 0)
                xcopies[i].start()

        @pl.when(not_facing)
        def _():
            for s, base in ((0, lay["up"]), (1, lay["down"])):
                gather(pool, both, base, ZFIRST, zn - ZFIRST, 2 * s * slots)
                zcopies[2 * s + 1].start()

        def inner(a):
            def put(f, total):
                acc[a * slots + f] = total

            totals(tab, a, 0, 6, 1, both, put)

        def pass_on(i):
            xcopies[i].wait_recv()
            ycopies[i].start()

        each(0, rows // 2, inner)

        @pl.when(facing)
        def _():
            pass_on(1)

        each(rows // 2, rows, inner)

        @pl.when(facing)
        def _():
            for i in range(2, early - 1):
                pass_on(i)
            for copy in zpass:
                copy.wait_recv()

            def one(j):
                code = tab[0, lay["pool"] + j]
                far = (code > PACK).astype(jnp.int32)
                a = both[lax.max(code - 1, 0) * (1 - far)].astype(jnp.float32)
                b = zone[(code - PACK - 1) * far].astype(jnp.float32)
                w = far.astype(jnp.float32)
                pool[j] = (a * (1.0 - w) + b * w).astype(pool.dtype)

            for i in range(early, len(parts)):
                lo, n = parts[i]
                each(lo, lo + n, one)
                xcopies[i].start()

        @pl.when(not_facing)
        def _():
            for s in range(2):
                for copy in zcopies[2 * s : 2 * s + 2]:
                    copy.wait_recv()
                zpass[s].start()

        def edge(e):
            a = e * (rows - 1)

            def put(f, total):
                acc[a * slots + f] += total

            totals(tab, a, 48, 2, 1, zone, put)

        each(0, 2, edge)

        @pl.when(facing)
        def _():
            for i in passed:
                if i >= early - 1:
                    pass_on(i)
            xcopies[0].wait_recv()
            for i in range(passed.stop, len(parts)):
                xcopies[i].wait_recv()

        @pl.when(not_facing)
        def _():
            for i in passed:
                ycopies[i].wait_recv()

        def last(a):
            def put(f, total):
                finish(a, f, acc[a * slots + f] + total)

            totals(tab, a, 64, 3, 3 if slots % 3 == 0 else 1, outer, put)

        each(0, rows, last)
        spread.wait_send()

        @pl.when(facing)
        def _():
            for copy in xcopies + [ycopies[i] for i in passed]:
                copy.wait_send()

        @pl.when(not_facing)
        def _():
            for copy in zcopies + zpass:
                copy.wait_send()

    def square(a, f, total):
        value = total.astype(squares.dtype)
        squares[a * slots + f] = value
        both2[a * slots + f] = value

    def step(a, f, total):
        used = tab1[a, lay["used"] + f].astype(jnp.float32)
        value = 1.5 * x[a * slots + f].astype(jnp.float32) - total * scale
        out[a * slots + f] = (value * used).astype(out.dtype)

    phase(0, tab1, x, both1, zone1, outer1, sizes[:4], square)
    phase(1, tab2, squares, both2, zone2, outer2, sizes[4:], step)


def local(x_blocks, columns, filter_ids):
    grps, ncol = lax.axis_size("grp"), lax.axis_size("col")
    rows, per_col, slots, order = x_blocks.shape[:4]
    assert per_col == 1 and filter_ids.shape[2] == slots and ncol % 4 == 0 and rows > 1
    grid_a, grid_c = rows * grps, ncol
    count = grid_a * grid_c
    held = rows * slots
    blocks = x_blocks.reshape(held, order, order)
    dtype = blocks.dtype
    full = (2 * held + FIRST, 3 * held, 3 * held, 2 * slots)
    levels = [s for s in STAIRS if max(s[:3] + s[4:7]) < full[0]] + [full + full]
    lay = layout(rows, slots)
    vmem = pl.BlockSpec(memory_space=pltpu.VMEM)
    smem = pl.BlockSpec(memory_space=pltpu.SMEM)
    table = jax.ShapeDtypeStruct((8, lay["width"]), jnp.int32)
    tab1, tab2, level = pl.pallas_call(
        functools.partial(plan_kernel, (rows, grid_a, grid_c, slots, levels)),
        out_shape=[table, table, jax.ShapeDtypeStruct((1,), jnp.int32)],
        in_specs=[vmem, vmem],
        out_specs=[vmem, vmem, smem],
        scratch_shapes=[
            pltpu.VMEM((lay["end"] - lay["up"], count), jnp.int32),
            pltpu.VMEM((lay["width"], 128), jnp.int32),
        ],
        name="plan",
    )(columns.transpose(2, 1, 0), filter_ids.transpose(2, 1, 0))

    def blocks_of(n):
        return pltpu.VMEM((n, order, order), dtype)

    branches = []
    for i, sizes in enumerate(levels):
        most1, most2 = sizes[2], sizes[6]
        parts = max(len(cut(*sizes[:3])), len(cut(*sizes[4:7])))
        dma = pltpu.SemaphoreType.DMA
        branches.append(
            pl.pallas_call(
                functools.partial(main_kernel, (rows, grid_c, slots), sizes, 0.5 / (slots * order)),
                out_shape=jax.ShapeDtypeStruct(blocks.shape, dtype),
                in_specs=[smem, smem, vmem],
                out_specs=vmem,
                scratch_shapes=[
                    blocks_of(2 * held + 1),
                    blocks_of(2 * held),
                    blocks_of(held),
                    blocks_of(4 * slots),
                    blocks_of(4 * slots),
                    blocks_of(most1),
                    blocks_of(most2),
                    blocks_of(max(most1, most2, 4 * slots)),
                    pltpu.VMEM((held, order, order), jnp.float32),
                    dma((2,)),
                    dma((2,)),
                    dma((2, 2, 2)),
                    dma((2, 2, 2)),
                    dma((2, 2)),
                    dma((2, 2)),
                    dma((2, parts)),
                    dma((2, parts)),
                    dma((2, parts)),
                ],
                compiler_params=pltpu.CompilerParams(
                    collective_id=i, has_side_effects=True, vmem_limit_bytes=LIMIT
                ),
                name="step_%d_%d" % (most1, most2),
            )
        )
    out = lax.switch(level[0], branches, tab1, tab2, blocks)
    return out.reshape(x_blocks.shape)


def solution(mesh):
    return jax.shard_map(
        local,
        mesh=mesh,
        in_specs=(P("grp", "col", None, None, None), P(), P()),
        out_specs=P("grp", "col", None, None, None),
        check_vma=False,
    )
```

```python
import functools

import jax
import jax.numpy as jnp
from jax import lax
from jax.experimental import pallas as pl
from jax.experimental.pallas import tpu as pltpu
from jax.sharding import PartitionSpec as P

MESH = pl.DeviceIdType.MESH
STEPS = [(da, dc) for da in (-1, 0, 1) for dc in (-1, 0, 1)]
EARLY, OWN = (0, 5), (5, 4)
ZEARLY, ZOWN = (0, 2), (2, 2)
LEAD = max(EARLY[0] + OWN[0], EARLY[1] + OWN[1])
PACK = 128
STAIRS = (
    (16, 21, 24, 7, 22, 29, 32, 10),
    (18, 24, 26, 8, 22, 28, 31, 10),
    (19, 24, 27, 8, 24, 31, 34, 11),
    (19, 26, 30, 8, 24, 31, 35, 11),
    (19, 25, 28, 10, 24, 31, 36, 11),
    (18, 24, 27, 8, 24, 31, 38, 13),
    (19, 26, 31, 10, 24, 31, 40, 13),
)
LIMIT = 59 * 1024 * 1024


def grid_maps(shape, grid_a, grid_c, rows):
    rid = lax.broadcasted_iota(jnp.int32, shape, 1)
    a = jnp.zeros_like(rid)
    for i in range(1, grid_a):
        a = a + (rid >= i * grid_c).astype(jnp.int32)
    group = jnp.zeros_like(rid)
    for i in range(1, grid_a // rows):
        group = group + (a >= i * rows).astype(jnp.int32)
    return rid, rid - a * grid_c, a - group * rows, group


def row_of(x, i):
    return jnp.broadcast_to(x[i : i + 1], x.shape)


def most_of(x):
    return jnp.broadcast_to(jnp.max(x, axis=0, keepdims=True), x.shape)


def sum_of(x):
    return jnp.broadcast_to(jnp.sum(x, axis=0, keepdims=True), x.shape)


def zone_half(slots):
    return 2 * slots + ZEARLY[1]


def layout(rows, slots):
    bases = {"terms": 0, "used": 88, "up": 96}
    bases["down"] = 96 + zone_half(slots)
    bases["pool"] = 96 + 2 * zone_half(slots)
    bases["end"] = bases["pool"] + 3 * rows * slots + LEAD
    bases["width"] = (bases["end"] + 127) // 128 * 128
    return bases


def plan_kernel(dims, cols_ref, filt_ref, tab1, tab2, level, lists, wide):
    rows, grid_a, grid_c, slots, levels = dims
    count = grid_a * grid_c
    held = rows * slots

    def roll(x, s, axis):
        s = s % x.shape[axis]
        return pltpu.roll(x, s, axis) if s else x

    shape = (8, count)
    rid, col, al, group = grid_maps(shape, grid_a, grid_c, rows)
    lane_row = lax.broadcasted_iota(jnp.int32, (grid_a, count), 1) // grid_c
    spread = (lane_row == lax.broadcasted_iota(jnp.int32, (grid_a, count), 0)).astype(jnp.float32)
    pick_col = lax.broadcasted_iota(jnp.int32, (grid_c, count), 1) % grid_c
    pick_col = pick_col == lax.broadcasted_iota(jnp.int32, (grid_c, count), 0)

    def laid(ref):
        flat = ref[...].reshape(slots * grid_c, grid_a).astype(jnp.float32)
        wide_ids = jnp.dot(flat, spread, precision=lax.Precision.HIGHEST, preferred_element_type=jnp.float32)
        sub = lax.broadcasted_iota(jnp.int32, shape, 0)
        ids = jnp.full(shape, -1, jnp.int32)
        for k in range(slots):
            part = jnp.where(pick_col, wide_ids[k * grid_c : (k + 1) * grid_c], 0.0)
            line = jnp.sum(part, axis=0, keepdims=True).astype(jnp.int32)
            ids = jnp.where(sub == k, jnp.broadcast_to(line, shape), ids)
        return ids

    cols, filt = laid(cols_ref), laid(filt_ref)
    sub = lax.broadcasted_iota(jnp.int32, cols.shape, 0)
    odd = lax.rem(col, 2) == 1
    quad = lax.rem(col, 4)
    facing = (quad == 1) | (quad == 2)
    low, high = al == 0, al == rows - 1

    def sh(x, step):
        da, dc = step
        x = roll(x, -da * grid_c, 1)
        if dc == 1:
            x = jnp.where(col == grid_c - 1, roll(x, grid_c - 1, 1), roll(x, -1, 1))
        if dc == -1:
            x = jnp.where(col == 0, roll(x, 1 - grid_c, 1), roll(x, 1, 1))
        return x

    def partner(x):
        return jnp.where(odd, roll(x, 1, 1), roll(x, -1, 1))

    def ahead_of(n):
        ahead = jnp.zeros_like(n)
        for s in range(1, slots):
            ahead = ahead + jnp.where(sub >= s, roll(n, s, 0), 0)
        return ahead

    def ranked(n):
        total = sum_of(n)
        before, after = jnp.zeros_like(n), jnp.zeros_like(n)
        for s in range(1, rows):
            before = before + jnp.where(al >= s, roll(total, s * grid_c, 1), 0)
            after = after + jnp.where(al < rows - s, roll(total, -s * grid_c, 1), 0)
        return before + ahead_of(n), before + total + after

    uses, kslot = [], []
    for step in STEPS:
        hit = (cols == sh(rid, step)).astype(jnp.int32)
        uses.append(most_of(hit))
        kslot.append(al * slots + sum_of(hit * sub))

    def early_of(stored, wanted):
        asked = jnp.where(wanted < 0, -2, wanted)
        late = jnp.zeros_like(stored)
        for i, (da, dc) in enumerate(STEPS):
            kept = sh(stored, (da, dc))
            found = jnp.zeros_like(stored)
            for m in range(slots):
                found = found | (asked == row_of(kept, m)).astype(jnp.int32)
            to = al + da
            away = (to < 0) | (to >= rows)
            if dc:
                away = away | (odd if dc == 1 else ~odd)
            late = late | (found & uses[i] & away.astype(jnp.int32))
        return 1 - late

    def lined(rank_of, mask, early, lead, n_early, n_own):
        erank, en = rank_of(mask & early)
        lrank, ln = rank_of(mask & (1 - early))
        rank, n = jnp.where(early > 0, erank, en + lrank), en + ln
        n_lead, n_tail = jnp.where(lead, n, partner(n)), jnp.where(lead, partner(n), n)
        taken = jnp.minimum(jnp.where(lead, en, partner(en)), n_early)
        also = taken + jnp.minimum(n_lead - taken, n_own)
        start = n_early + n_own
        place = jnp.where(rank < also, n_early + rank - taken, start + n_tail + rank - also)
        place = jnp.where(rank < taken, rank, place)
        return jnp.where(lead, place, start + rank), start + n_tail + n_lead - also, n_tail

    def needs(stored, wanted, early, which):
        asked = jnp.where(wanted < 0, -2, wanted)
        need = {(gd, dc): jnp.zeros_like(stored) for gd in (-1, 0, 1) for dc in (-1, 0, 1)}
        for i, (da, dc) in enumerate(STEPS):
            back = (-da, -dc)
            there = sh(asked, back)
            hit = jnp.zeros_like(stored)
            for f in range(slots):
                hit = hit | (stored == row_of(there, f)).astype(jnp.int32)
            hit = hit & sh(uses[i], back)
            at = al - da
            if dc:
                inside = ((at >= 0) & (at < rows)).astype(jnp.int32)
                need[0, -dc] = need[0, -dc] | (hit & inside)
            if da == -1:
                need[1, -dc] = need[1, -dc] | (hit & high.astype(jnp.int32))
            if da == 1:
                need[-1, -dc] = need[-1, -dc] | (hit & low.astype(jnp.int32))
        flat = jnp.where(odd, need[0, 1], need[0, -1])
        ups = need[1, 0] | need[1, 1] | need[1, -1]
        downs = need[-1, 0] | need[-1, 1] | need[-1, -1]
        corner = roll(jnp.where(odd, need[1, 1], need[1, -1]), grid_c, 1)
        corner = corner | roll(jnp.where(odd, need[-1, 1], need[-1, -1]), -grid_c, 1)
        rank, n_in, n_far = lined(ranked, flat, early, facing, EARLY[which], OWN[which])
        crank, cn = ranked(corner)
        cother = partner(cn)
        c_near, c_far = jnp.where(facing, cn, cother), jnp.where(facing, cother, cn)
        zups, zdowns, zmost = [], [], []
        for lists_of, src in ((zups, ups), (zdowns, downs)):
            spot, total, _ = lined(
                lambda x: (ahead_of(x), sum_of(x)), src, early, ~facing, ZEARLY[which], ZOWN[which]
            )
            lists_of.append(spot)
            zmost.append(jnp.max(total))
        z_most = jnp.maximum(zmost[0], zmost[1])
        return {
            "wanted": asked,
            "flat": flat,
            "rank": rank,
            "corner": corner,
            "crank": crank,
            "n_in": n_in,
            "n_far": n_far,
            "c_near": c_near,
            "c_far": c_far,
            "ups": ups,
            "downs": downs,
            "zup": zups[0],
            "zdown": zdowns[0],
            "z_most": z_most,
        }

    first = needs(cols, filt, jnp.ones_like(cols), 0)
    second = needs(filt, cols, early_of(cols, filt), 1)
    pick, failed = jnp.int32(0), jnp.int32(1)
    before = [jnp.int32(levels[0][0]), jnp.int32(levels[0][4])]
    for i, step in enumerate(levels[:-1]):
        over = jnp.bool_(False)
        for j, data in enumerate((first, second)):
            at, reach, most, zn = step[4 * j : 4 * j + 4]
            total = jnp.maximum(data["n_in"], at) + data["c_near"] + data["c_far"]
            passed = jnp.maximum(data["n_far"] + EARLY[j] + OWN[j], at) + data["c_far"]
            over = over | (jnp.max(total) > most) | (jnp.max(passed) > reach) | (data["z_most"] > zn)
        failed = failed * over.astype(jnp.int32)
        pick = pick + failed
        for j in range(2):
            before[j] = jnp.where(failed > 0, levels[i + 1][4 * j], before[j])
    level[0] = pick

    grp, me = lax.axis_index("grp"), lax.axis_index("col")
    start = grp * rows * grid_c + me
    chip = (group == grp) & ((col - lax.rem(col, 2)) == (me - lax.rem(me, 2)))
    absent = jnp.full_like(al, 2 * held * PACK)
    lay = layout(rows, slots)

    def here(x):
        return pltpu.roll(x, count - start, 1)[:, :128]

    def write(tab, stored, data, at, lead):
        absent_far = absent + lead
        wanted = data["wanted"]
        rank = data["rank"] + jnp.where(data["rank"] >= at, data["c_far"], 0)
        crank = data["crank"] + jnp.where(facing, jnp.maximum(data["n_in"], at) + data["c_far"], at)
        zpos = jnp.where(low, roll(data["zup"], grid_c, 1), zone_half(slots) + roll(data["zdown"], -grid_c, 1))
        own = al * slots + sub
        codes = {}
        for i, (da, dc) in enumerate(STEPS):
            to = al + da
            inside = (to >= 0) & (to < rows)
            flat_at = sh(own, (da, dc))
            z_at = sh(zpos, (0, dc))
            none = absent
            if dc:
                outer = odd if dc == 1 else ~odd
                flat_at = jnp.where(outer, sh(rank, (da, dc)), held + flat_at)
                z_at = jnp.where(outer, sh(crank, (0, dc)), z_at)
                none = jnp.where(outer, absent_far, absent)
            place = jnp.where(inside, flat_at, z_at)
            kept = sh(stored, (da, dc))
            found = jnp.full_like(own, -1)
            for m in range(slots):
                found = jnp.where(wanted == row_of(kept, m), row_of(place, m), found)
            ok = (found >= 0) & (uses[i] > 0)
            codes[da, dc] = jnp.where(ok, kslot[i] * PACK + found, none)
        for da in (-1, 0, 1):
            to = al + da
            inside = (to >= 0) & (to < rows)
            near = jnp.where(odd, codes[da, -1], codes[da, 1])
            far = jnp.where(odd, codes[da, 1], codes[da, -1])
            for j, x in ((0, codes[da, 0]), (1, near)):
                at_row = (j * 3 + da + 1) * 8
                wide[at_row : at_row + 8, :] = here(jnp.where(inside, x, absent))
            at_row = (8 + da + 1) * 8
            wide[at_row : at_row + 8, :] = here(far)
        for j in range(2):
            pair = []
            for da in (-1, 1):
                near = jnp.where(odd, codes[da, -1], codes[da, 1])
                pair.append(codes[da, 0] if j == 0 else near)
            z = jnp.where(low, pair[0], jnp.where(high, pair[1], absent))
            wide[(6 + j) * 8 : (7 + j) * 8, :] = here(z)
        wide[lay["used"] : lay["used"] + 8, :] = here((cols >= 0).astype(jnp.int32))
        side = jnp.where(col == me, 0, 1)
        block = own + side * held + 1
        flat_code = jnp.where(chip & (data["flat"] > 0), block, 0)
        corner_code = jnp.where(chip & (data["corner"] > 0), PACK + zpos + 1, 0)
        up_code = jnp.where(chip & (data["ups"] > 0), block, 0)
        down_code = jnp.where(chip & (data["downs"] > 0), block, 0)
        base = lay["up"]

        def put(row, x):
            lists[row - base : row - base + 1, :] = jnp.max(x, axis=0, keepdims=True)

        for j in range(zone_half(slots)):
            put(lay["up"] + j, jnp.where(data["zup"] == j, up_code, 0))
            put(lay["down"] + j, jnp.where(data["zdown"] == j, down_code, 0))
        for j in range(lay["end"] - lay["pool"]):
            x = jnp.where(rank == j, flat_code, 0)
            put(lay["pool"] + j, jnp.maximum(x, jnp.where(crank == j, corner_code, 0)))
        found = jnp.max(lists[...], axis=1, keepdims=True)
        wide[base : lay["end"], :] = jnp.broadcast_to(found, (lay["end"] - base, 128))
        turned = wide[...].T
        for a in range(rows):
            tab[a : a + 1, :] = turned[a * grid_c : a * grid_c + 1, :]

    write(tab1, cols, first, before[0], EARLY[0] + OWN[0])
    write(tab2, filt, second, before[1], EARLY[1] + OWN[1])


def pieces(start, stop, most):
    out = []
    while start < stop:
        n = min(most, stop - start)
        out.append((start, n))
        start += n
    return out


def cut(at, split, reach, most):
    lead = EARLY[at] + OWN[at]
    out = [(0, EARLY[at])] * (EARLY[at] > 0) + [(EARLY[at], OWN[at])]
    return out + pieces(lead, split, 2) + pieces(split, reach, 2) + pieces(reach, most, 4)


def main_kernel(
    dims,
    sizes,
    scale,
    tab1,
    tab2,
    x_ref,
    out_ref,
    both1,
    both2,
    squares,
    zone1,
    zone2,
    outer1,
    outer2,
    pool,
    ahead,
    acc,
    isem,
    dsend,
    drecv,
    zs_sem,
    zr_sem,
    zf_send,
    zf_recv,
    xs_sem,
    xr_sem,
    ys_sem,
):
    rows, grid_c, slots = dims
    held = rows * slots
    half = zone_half(slots)
    lay = layout(rows, slots)
    grp, col = lax.axis_index("grp"), lax.axis_index("col")
    grps = lax.axis_size("grp")
    quad = lax.rem(col, 4)
    odd = lax.rem(col, 2)
    facing = (quad == 1) | (quad == 2)
    sign = 1 - 2 * odd
    partner = (grp, col + sign)
    above = (lax.rem(grp + 1, grps), col)
    below = (lax.rem(grp + grps - 1, grps), col)
    across = (grp, lax.rem(col - sign + grid_c, grid_c))
    relay = (grp, lax.rem(col - 3 * sign + grid_c, grid_c))

    loads = [
        pltpu.make_async_copy(x_ref, squares, isem.at[0]),
        pltpu.make_async_copy(x_ref, both1.at[pl.ds(0, held)], isem.at[1]),
    ]
    for load in loads:
        load.start()
    barrier = pltpu.get_barrier_semaphore()
    for peer in (partner, relay):
        pl.semaphore_signal(barrier, inc=1, device_id=peer, device_id_type=MESH)

    @pl.when(facing)
    def _():
        pl.semaphore_signal(barrier, inc=1, device_id=across, device_id_type=MESH)
        pl.semaphore_wait(barrier, 3)

    @pl.when(jnp.logical_not(facing))
    def _():
        for peer in (above, below):
            pl.semaphore_signal(barrier, inc=1, device_id=peer, device_id_type=MESH)
        pl.semaphore_wait(barrier, 4)

    def remote(src, dst, send_sem, recv_sem, peer):
        return pltpu.make_async_remote_copy(
            src_ref=src, dst_ref=dst, send_sem=send_sem, recv_sem=recv_sem, device_id=peer, device_id_type=MESH
        )

    def each(lo, hi, body):
        def one(i, carry):
            body(i)
            return carry

        lax.fori_loop(lo, hi, one, 0)

    def product(tab, row, a, right):
        code = tab[a, row]
        return jnp.dot(
            both1[lax.div(code, PACK)], right[lax.rem(code, PACK)], preferred_element_type=jnp.float32
        )

    def totals(tab, a, base, terms, wide, right, put):
        def one(i, carry):
            sums = [None] * wide
            for j in range(terms):
                for q in range(wide):
                    term = product(tab, base + j * 8 + i * wide + q, a, right)
                    sums[q] = term if sums[q] is None else sums[q] + term
            for q in range(wide):
                put(i * wide + q, sums[q])
            return carry

        lax.fori_loop(0, slots // wide, one, 0)

    def phase(at, tab, src, both, zone, outer, sizes, early_x, early_z, finish):
        split, reach, most, zn = sizes
        not_facing = jnp.logical_not(facing)
        spread = remote(src, both.at[pl.ds(held, held)], dsend.at[at], drecv.at[at], partner)
        spread.start()
        parts = cut(at, split, reach, most)
        n_lead = 1 + (EARLY[at] > 0)
        lead = EARLY[at] + OWN[at]
        xcopies, ycopies = [], []
        for i, (lo, n) in enumerate(parts):
            place = outer.at[pl.ds(lo, n)]
            held_at = ahead.at[pl.ds(0, n)] if i < n_lead - 1 else pool.at[pl.ds(lo, n)]
            xcopies.append(remote(held_at, place, xs_sem.at[at, i], xr_sem.at[at, i], across))
            passing = lead <= lo < reach
            ycopies.append(remote(place, place, ys_sem.at[at, i], xr_sem.at[at, i], relay) if passing else None)
        early = sum(lo < split for lo, _ in parts)
        passed = range(n_lead, sum(lo < reach for lo, _ in parts))
        zlead = ZEARLY[at] + ZOWN[at]
        zcopies, zpass = [[], []], []
        for s, peer in ((0, above), (1, below)):
            for i, (lo, n) in enumerate(((0, ZEARLY[at]), (ZEARLY[at], ZOWN[at]), (zlead, zn - zlead))):
                if n:
                    held_at = ahead.at[pl.ds(s * n, n)] if i == 0 else pool.at[pl.ds(s * half + lo, n)]
                    sems = zs_sem.at[at, s, i], zr_sem.at[at, s, i]
                    zcopies[s].append(remote(held_at, zone.at[pl.ds(s * half + lo, n)], *sems, peer))
            piece = pl.ds(s * half, zn)
            zpass.append(remote(zone.at[piece], zone.at[piece], zf_send.at[at, s], zf_recv.at[at, s], partner))

        def gather(dst, src, base, lo, n, to):
            def one(j):
                dst[to + j] = src[lax.max(tab[0, base + j] - 1, 0)]

            each(lo, lo + n, one)

        @pl.when(facing)
        def _():
            gather(pool, src, lay["pool"], EARLY[at], OWN[at], 0)
            xcopies[n_lead - 1].start()

        @pl.when(not_facing)
        def _():
            for s, base in ((0, lay["up"]), (1, lay["down"])):
                gather(pool, src, base, ZEARLY[at], ZOWN[at], s * half)
                zcopies[s][-2].start()

        if at == 0:
            loads[1].wait()
            both[2 * held] = jnp.zeros(both.shape[1:], both.dtype)
        spread.wait_recv()

        @pl.when(facing)
        def _():
            for i in range(n_lead, early):
                gather(pool, both, lay["pool"], *parts[i], 0)
                xcopies[i].start()

        @pl.when(not_facing)
        def _():
            for s, base in ((0, lay["up"]), (1, lay["down"])):
                gather(pool, both, base, zlead, zn - zlead, s * half)
                zcopies[s][-1].start()

        def inner(a):
            def put(f, total):
                acc[a * slots + f] = total

            totals(tab, a, 0, 6, 1, both, put)

        def pass_on(i):
            xcopies[i].wait_recv()
            ycopies[i].start()

        woven = min(rows, early - n_lead - 1)

        def weave(a):
            inner(a)

            @pl.when(facing & (a < woven))
            def _():
                place = outer.at[pl.ds(lead + 2 * a, 2)]
                sems = ys_sem.at[at, n_lead + a], xr_sem.at[at, n_lead + a]
                remote(pool.at[pl.ds(lead + 2 * a, 2)], place, xs_sem.at[at, n_lead + a], sems[1], across).wait_recv()
                remote(place, place, *sems, relay).start()

        each(0, rows, weave)

        @pl.when(facing)
        def _():
            for i in range(n_lead + woven, early - 1):
                pass_on(i)
            for copy in zpass:
                copy.wait_recv()

            def one(j):
                code = tab[0, lay["pool"] + j]
                far = (code > PACK).astype(jnp.int32)
                a = both[lax.max(code - 1, 0) * (1 - far)].astype(jnp.float32)
                b = zone[(code - PACK - 1) * far].astype(jnp.float32)
                w = far.astype(jnp.float32)
                pool[j] = (a * (1.0 - w) + b * w).astype(pool.dtype)

            for i in range(early, len(parts)):
                lo, n = parts[i]
                each(lo, lo + n, one)
                xcopies[i].start()
            early_x()

        @pl.when(not_facing)
        def _():
            early_z()
            for s in range(2):
                for copy in zcopies[s]:
                    copy.wait_recv()
                zpass[s].start()

        def edge(e):
            a = e * (rows - 1)

            def put(f, total):
                acc[a * slots + f] += total

            totals(tab, a, 48, 2, 1, zone, put)

        each(0, 2, edge)

        @pl.when(facing)
        def _():
            for i in passed:
                if i >= max(early - 1, n_lead + woven):
                    pass_on(i)
            for i in range(n_lead):
                xcopies[i].wait_recv()
            for i in range(passed.stop, len(parts)):
                xcopies[i].wait_recv()

        @pl.when(not_facing)
        def _():
            for i in passed:
                ycopies[i].wait_recv()

        def last(a):
            def put(f, total):
                finish(a, f, acc[a * slots + f] + total)

            totals(tab, a, 64, 3, 3 if slots % 3 == 0 else 1, outer, put)

        spread.wait_send()
        each(0, rows, last)

        @pl.when(facing)
        def _():
            for copy in xcopies + [ycopies[i] for i in passed]:
                copy.wait_send()

        @pl.when(not_facing)
        def _():
            for copy in zcopies[0] + zcopies[1] + zpass:
                copy.wait_send()

    def square(a, f, total):
        value = total.astype(squares.dtype)
        squares[a * slots + f] = value
        both2[a * slots + f] = value

    def step(a, f, total):
        used = tab1[a, lay["used"] + f].astype(jnp.float32)
        value = 1.5 * both1[a * slots + f].astype(jnp.float32) - total * scale
        out_ref[a * slots + f] = (value * used).astype(out_ref.dtype)

    def take(to, row, n):
        def one(j):
            ahead[to + j] = acc[lax.max(tab2[0, row + j] - 1, 0)].astype(ahead.dtype)

        each(0, n, one)

    def early_x():
        take(0, lay["pool"], EARLY[1])
        place = outer2.at[pl.ds(0, EARLY[1])]
        remote(ahead.at[pl.ds(0, EARLY[1])], place, xs_sem.at[1, 0], xr_sem.at[1, 0], across).start()

    def early_z():
        n = ZEARLY[1]
        for s, base, peer in ((0, lay["up"], above), (1, lay["down"], below)):
            take(s * n, base, n)
            place = zone2.at[pl.ds(s * half, n)]
            remote(ahead.at[pl.ds(s * n, n)], place, zs_sem.at[1, s, 0], zr_sem.at[1, s, 0], peer).start()

    loads[0].wait()
    phase(0, tab1, squares, both1, zone1, outer1, sizes[:4], early_x, early_z, square)
    nothing = lambda: None
    phase(1, tab2, squares, both2, zone2, outer2, sizes[4:], nothing, nothing, step)


def local(x_blocks, columns, filter_ids):
    grps, ncol = lax.axis_size("grp"), lax.axis_size("col")
    rows, per_col, slots, order = x_blocks.shape[:4]
    assert per_col == 1 and filter_ids.shape[2] == slots and ncol % 4 == 0 and rows > 1
    grid_a, grid_c = rows * grps, ncol
    count = grid_a * grid_c
    held = rows * slots
    blocks = x_blocks.reshape(held, order, order)
    dtype = blocks.dtype
    full = ()
    for n in EARLY:
        full += (2 * held + n, 2 * held + n + 4 * slots, 2 * held + n + 4 * slots, zone_half(slots))
    levels = [s for s in STAIRS if max(s[:3] + s[4:7]) < full[0]] + [full]
    lay = layout(rows, slots)
    vmem = pl.BlockSpec(memory_space=pltpu.VMEM)
    smem = pl.BlockSpec(memory_space=pltpu.SMEM)
    anyw = pl.BlockSpec(memory_space=pl.ANY)
    table = jax.ShapeDtypeStruct((8, lay["width"]), jnp.int32)
    tab1, tab2, level = pl.pallas_call(
        functools.partial(plan_kernel, (rows, grid_a, grid_c, slots, levels)),
        out_shape=[table, table, jax.ShapeDtypeStruct((1,), jnp.int32)],
        in_specs=[vmem, vmem],
        out_specs=[vmem, vmem, smem],
        scratch_shapes=[
            pltpu.VMEM((lay["end"] - lay["up"], count), jnp.int32),
            pltpu.VMEM((lay["width"], 128), jnp.int32),
        ],
        name="plan",
    )(columns.transpose(2, 1, 0), filter_ids.transpose(2, 1, 0))

    def blocks_of(n):
        return pltpu.VMEM((n, order, order), dtype)

    branches = []
    for i, sizes in enumerate(levels):
        most1, most2 = sizes[2], sizes[6]
        parts = max(len(cut(0, *sizes[:3])), len(cut(1, *sizes[4:7])))
        dma = pltpu.SemaphoreType.DMA
        branches.append(
            pl.pallas_call(
                functools.partial(main_kernel, (rows, grid_c, slots), sizes, 0.5 / (slots * order)),
                out_shape=pltpu.VMEM(blocks.shape, dtype),
                in_specs=[smem, smem, anyw],
                out_specs=vmem,
                scratch_shapes=[
                    blocks_of(2 * held + 1),
                    blocks_of(2 * held),
                    blocks_of(held),
                    blocks_of(2 * zone_half(slots)),
                    blocks_of(2 * zone_half(slots)),
                    blocks_of(most1),
                    blocks_of(most2),
                    blocks_of(max(most1, most2, 2 * zone_half(slots))),
                    blocks_of(max(EARLY[1], 2 * ZEARLY[1])),
                    pltpu.VMEM((held, order, order), jnp.float32),
                    dma((2,)),
                    dma((2,)),
                    dma((2,)),
                    dma((2, 2, 3)),
                    dma((2, 2, 3)),
                    dma((2, 2)),
                    dma((2, 2)),
                    dma((2, parts)),
                    dma((2, parts)),
                    dma((2, parts)),
                ],
                compiler_params=pltpu.CompilerParams(
                    collective_id=i, has_side_effects=True, vmem_limit_bytes=LIMIT
                ),
                name="step_%d_%d" % (most1, most2),
            )
        )
    out = lax.switch(level[0], branches, tab1, tab2, blocks)
    return out.reshape(x_blocks.shape)


def solution(mesh):
    return jax.shard_map(
        local,
        mesh=mesh,
        in_specs=(P("grp", "col", None, None, None), P(), P()),
        out_specs=P("grp", "col", None, None, None),
        check_vma=False,
    )
```

```python
import functools

import jax
import jax.numpy as jnp
from jax import lax
from jax.experimental import pallas as pl
from jax.experimental.pallas import tpu as pltpu
from jax.sharding import PartitionSpec as P

MESH = pl.DeviceIdType.MESH
STEPS = [(da, dc) for da in (-1, 0, 1) for dc in (-1, 0, 1)]
EARLY, OWN = (0, 5), (5, 4)
ZEARLY, ZOWN = (0, 2), (2, 2)
LEAD = max(EARLY[0] + OWN[0], EARLY[1] + OWN[1])
PACK = 128
STAIRS = (
    (17, 21, 25, 7, 24, 29, 33, 10),
    (17, 22, 26, 7, 24, 30, 34, 10),
    (19, 24, 28, 8, 24, 30, 34, 10),
    (19, 23, 27, 8, 26, 32, 36, 11),
    (19, 24, 28, 8, 26, 33, 38, 11),
    (19, 25, 30, 9, 26, 32, 36, 11),
    (19, 24, 28, 9, 26, 33, 40, 13),
    (19, 26, 31, 10, 26, 33, 38, 12),
)
LIMIT = 59 * 1024 * 1024


def grid_maps(shape, grid_a, grid_c, rows):
    rid = lax.broadcasted_iota(jnp.int32, shape, 1)
    a = jnp.zeros_like(rid)
    for i in range(1, grid_a):
        a = a + (rid >= i * grid_c).astype(jnp.int32)
    group = jnp.zeros_like(rid)
    for i in range(1, grid_a // rows):
        group = group + (a >= i * rows).astype(jnp.int32)
    return rid, rid - a * grid_c, a - group * rows, group


def row_of(x, i):
    return jnp.broadcast_to(x[i : i + 1], x.shape)


def most_of(x):
    return jnp.broadcast_to(jnp.max(x, axis=0, keepdims=True), x.shape)


def sum_of(x):
    return jnp.broadcast_to(jnp.sum(x, axis=0, keepdims=True), x.shape)


def zone_half(slots):
    return 2 * slots + ZEARLY[1]


def layout(rows, slots):
    bases = {"terms": 0, "used": 88, "up": 96}
    bases["down"] = 96 + zone_half(slots)
    bases["pool"] = 96 + 2 * zone_half(slots)
    bases["end"] = bases["pool"] + 3 * rows * slots + LEAD
    bases["width"] = (bases["end"] + 127) // 128 * 128
    return bases


def plan_kernel(dims, cols_ref, filt_ref, tab1, tab2, level, lists, wide):
    rows, grid_a, grid_c, slots, levels = dims
    count = grid_a * grid_c
    held = rows * slots

    def roll(x, s, axis):
        s = s % x.shape[axis]
        return pltpu.roll(x, s, axis) if s else x

    shape = (8, count)
    rid, col, al, group = grid_maps(shape, grid_a, grid_c, rows)
    lane_row = lax.broadcasted_iota(jnp.int32, (grid_a, count), 1) // grid_c
    spread = (lane_row == lax.broadcasted_iota(jnp.int32, (grid_a, count), 0)).astype(jnp.float32)
    pick_col = lax.broadcasted_iota(jnp.int32, (grid_c, count), 1) % grid_c
    pick_col = pick_col == lax.broadcasted_iota(jnp.int32, (grid_c, count), 0)

    def laid(ref):
        flat = ref[...].reshape(slots * grid_c, grid_a).astype(jnp.float32)
        wide_ids = jnp.dot(flat, spread, precision=lax.Precision.HIGHEST, preferred_element_type=jnp.float32)
        sub = lax.broadcasted_iota(jnp.int32, shape, 0)
        ids = jnp.full(shape, -1, jnp.int32)
        for k in range(slots):
            part = jnp.where(pick_col, wide_ids[k * grid_c : (k + 1) * grid_c], 0.0)
            line = jnp.sum(part, axis=0, keepdims=True).astype(jnp.int32)
            ids = jnp.where(sub == k, jnp.broadcast_to(line, shape), ids)
        return ids

    cols, filt = laid(cols_ref), laid(filt_ref)
    sub = lax.broadcasted_iota(jnp.int32, cols.shape, 0)
    odd = lax.rem(col, 2) == 1
    quad = lax.rem(col, 4)
    facing = (quad == 1) | (quad == 2)
    low, high = al == 0, al == rows - 1

    def sh(x, step):
        da, dc = step
        x = roll(x, -da * grid_c, 1)
        if dc == 1:
            x = jnp.where(col == grid_c - 1, roll(x, grid_c - 1, 1), roll(x, -1, 1))
        if dc == -1:
            x = jnp.where(col == 0, roll(x, 1 - grid_c, 1), roll(x, 1, 1))
        return x

    def partner(x):
        return jnp.where(odd, roll(x, 1, 1), roll(x, -1, 1))

    def ahead_of(n):
        ahead = jnp.zeros_like(n)
        for s in range(1, slots):
            ahead = ahead + jnp.where(sub >= s, roll(n, s, 0), 0)
        return ahead

    def ranked(n):
        total = sum_of(n)
        before, after = jnp.zeros_like(n), jnp.zeros_like(n)
        for s in range(1, rows):
            before = before + jnp.where(al >= s, roll(total, s * grid_c, 1), 0)
            after = after + jnp.where(al < rows - s, roll(total, -s * grid_c, 1), 0)
        return before + ahead_of(n), before + total + after

    uses, kslot = [], []
    for step in STEPS:
        hit = (cols == sh(rid, step)).astype(jnp.int32)
        uses.append(most_of(hit))
        kslot.append(al * slots + sum_of(hit * sub))

    def early_of(stored, wanted):
        asked = jnp.where(wanted < 0, -2, wanted)
        late = jnp.zeros_like(stored)
        for i, (da, dc) in enumerate(STEPS):
            kept = sh(stored, (da, dc))
            found = jnp.zeros_like(stored)
            for m in range(slots):
                found = found | (asked == row_of(kept, m)).astype(jnp.int32)
            to = al + da
            away = (to < 0) | (to >= rows)
            if dc:
                away = away | (odd if dc == 1 else ~odd)
            late = late | (found & uses[i] & away.astype(jnp.int32))
        return 1 - late

    def lined(rank_of, mask, early, lead, n_early, n_own):
        erank, en = rank_of(mask & early)
        lrank, ln = rank_of(mask & (1 - early))
        rank, n = jnp.where(early > 0, erank, en + lrank), en + ln
        n_lead, n_tail = jnp.where(lead, n, partner(n)), jnp.where(lead, partner(n), n)
        taken = jnp.minimum(jnp.where(lead, en, partner(en)), n_early)
        also = taken + jnp.minimum(n_lead - taken, n_own)
        start = n_early + n_own
        place = jnp.where(rank < also, n_early + rank - taken, start + n_tail + rank - also)
        place = jnp.where(rank < taken, rank, place)
        return jnp.where(lead, place, start + rank), start + n_tail + n_lead - also, n_tail

    def needs(stored, wanted, early, which):
        asked = jnp.where(wanted < 0, -2, wanted)
        need = {(gd, dc): jnp.zeros_like(stored) for gd in (-1, 0, 1) for dc in (-1, 0, 1)}
        for i, (da, dc) in enumerate(STEPS):
            back = (-da, -dc)
            there = sh(asked, back)
            hit = jnp.zeros_like(stored)
            for f in range(slots):
                hit = hit | (stored == row_of(there, f)).astype(jnp.int32)
            hit = hit & sh(uses[i], back)
            at = al - da
            if dc:
                inside = ((at >= 0) & (at < rows)).astype(jnp.int32)
                need[0, -dc] = need[0, -dc] | (hit & inside)
            if da == -1:
                need[1, -dc] = need[1, -dc] | (hit & high.astype(jnp.int32))
            if da == 1:
                need[-1, -dc] = need[-1, -dc] | (hit & low.astype(jnp.int32))
        flat = jnp.where(odd, need[0, 1], need[0, -1])
        ups = need[1, 0] | need[1, 1] | need[1, -1]
        downs = need[-1, 0] | need[-1, 1] | need[-1, -1]
        corner = roll(jnp.where(odd, need[1, 1], need[1, -1]), grid_c, 1)
        corner = corner | roll(jnp.where(odd, need[-1, 1], need[-1, -1]), -grid_c, 1)
        rank, n_in, n_far = lined(ranked, flat, early, facing, EARLY[which], OWN[which])
        crank, cn = ranked(corner)
        cother = partner(cn)
        c_near, c_far = jnp.where(facing, cn, cother), jnp.where(facing, cother, cn)
        zups, zdowns, zmost = [], [], []
        for lists_of, src in ((zups, ups), (zdowns, downs)):
            spot, total, _ = lined(
                lambda x: (ahead_of(x), sum_of(x)), src, early, ~facing, ZEARLY[which], ZOWN[which]
            )
            lists_of.append(spot)
            zmost.append(jnp.max(total))
        z_most = jnp.maximum(zmost[0], zmost[1])
        return {
            "wanted": asked,
            "flat": flat,
            "rank": rank,
            "corner": corner,
            "crank": crank,
            "n_in": n_in,
            "n_far": n_far,
            "c_near": c_near,
            "c_far": c_far,
            "ups": ups,
            "downs": downs,
            "zup": zups[0],
            "zdown": zdowns[0],
            "z_most": z_most,
        }

    first = needs(cols, filt, jnp.ones_like(cols), 0)
    second = needs(filt, cols, early_of(cols, filt), 1)
    pick, failed = jnp.int32(0), jnp.int32(1)
    before = [jnp.int32(levels[0][0]), jnp.int32(levels[0][4])]
    for i, step in enumerate(levels[:-1]):
        over = jnp.bool_(False)
        for j, data in enumerate((first, second)):
            at, reach, most, zn = step[4 * j : 4 * j + 4]
            total = jnp.maximum(data["n_in"], at) + data["c_near"] + data["c_far"]
            passed = jnp.maximum(data["n_far"] + EARLY[j] + OWN[j], at) + data["c_far"]
            over = over | (jnp.max(total) > most) | (jnp.max(passed) > reach) | (data["z_most"] > zn)
        failed = failed * over.astype(jnp.int32)
        pick = pick + failed
        for j in range(2):
            before[j] = jnp.where(failed > 0, levels[i + 1][4 * j], before[j])
    level[0] = pick

    grp, me = lax.axis_index("grp"), lax.axis_index("col")
    start = grp * rows * grid_c + me
    chip = (group == grp) & ((col - lax.rem(col, 2)) == (me - lax.rem(me, 2)))
    absent = jnp.full_like(al, 2 * held * PACK)
    lay = layout(rows, slots)

    def here(x):
        return pltpu.roll(x, count - start, 1)[:, :128]

    def write(tab, stored, data, at, lead):
        absent_far = absent + lead
        wanted = data["wanted"]
        rank = data["rank"] + jnp.where(data["rank"] >= at, data["c_far"], 0)
        crank = data["crank"] + jnp.where(facing, jnp.maximum(data["n_in"], at) + data["c_far"], at)
        zpos = jnp.where(low, roll(data["zup"], grid_c, 1), zone_half(slots) + roll(data["zdown"], -grid_c, 1))
        own = al * slots + sub
        codes = {}
        for i, (da, dc) in enumerate(STEPS):
            to = al + da
            inside = (to >= 0) & (to < rows)
            flat_at = sh(own, (da, dc))
            z_at = sh(zpos, (0, dc))
            none = absent
            if dc:
                outer = odd if dc == 1 else ~odd
                flat_at = jnp.where(outer, sh(rank, (da, dc)), held + flat_at)
                z_at = jnp.where(outer, sh(crank, (0, dc)), z_at)
                none = jnp.where(outer, absent_far, absent)
            place = jnp.where(inside, flat_at, z_at)
            kept = sh(stored, (da, dc))
            found = jnp.full_like(own, -1)
            for m in range(slots):
                found = jnp.where(wanted == row_of(kept, m), row_of(place, m), found)
            ok = (found >= 0) & (uses[i] > 0)
            codes[da, dc] = jnp.where(ok, kslot[i] * PACK + found, none)
        for da in (-1, 0, 1):
            to = al + da
            inside = (to >= 0) & (to < rows)
            near = jnp.where(odd, codes[da, -1], codes[da, 1])
            far = jnp.where(odd, codes[da, 1], codes[da, -1])
            for j, x in ((0, codes[da, 0]), (1, near)):
                at_row = (j * 3 + da + 1) * 8
                wide[at_row : at_row + 8, :] = here(jnp.where(inside, x, absent))
            at_row = (8 + da + 1) * 8
            wide[at_row : at_row + 8, :] = here(far)
        for j in range(2):
            pair = []
            for da in (-1, 1):
                near = jnp.where(odd, codes[da, -1], codes[da, 1])
                pair.append(codes[da, 0] if j == 0 else near)
            z = jnp.where(low, pair[0], jnp.where(high, pair[1], absent))
            wide[(6 + j) * 8 : (7 + j) * 8, :] = here(z)
        wide[lay["used"] : lay["used"] + 8, :] = here((cols >= 0).astype(jnp.int32))
        side = jnp.where(col == me, 0, 1)
        block = own + side * held + 1
        flat_code = jnp.where(chip & (data["flat"] > 0), block, 0)
        corner_code = jnp.where(chip & (data["corner"] > 0), PACK + zpos + 1, 0)
        up_code = jnp.where(chip & (data["ups"] > 0), block, 0)
        down_code = jnp.where(chip & (data["downs"] > 0), block, 0)
        base = lay["up"]

        def put(row, x):
            lists[row - base : row - base + 1, :] = jnp.max(x, axis=0, keepdims=True)

        for j in range(zone_half(slots)):
            put(lay["up"] + j, jnp.where(data["zup"] == j, up_code, 0))
            put(lay["down"] + j, jnp.where(data["zdown"] == j, down_code, 0))
        for j in range(lay["end"] - lay["pool"]):
            x = jnp.where(rank == j, flat_code, 0)
            put(lay["pool"] + j, jnp.maximum(x, jnp.where(crank == j, corner_code, 0)))
        found = jnp.max(lists[...], axis=1, keepdims=True)
        wide[base : lay["end"], :] = jnp.broadcast_to(found, (lay["end"] - base, 128))
        turned = wide[...].T
        for a in range(rows):
            tab[a : a + 1, :] = turned[a * grid_c : a * grid_c + 1, :]

    write(tab1, cols, first, before[0], EARLY[0] + OWN[0])
    write(tab2, filt, second, before[1], EARLY[1] + OWN[1])


def pieces(start, stop, most):
    out = []
    while start < stop:
        n = min(most, stop - start)
        out.append((start, n))
        start += n
    return out


def cut(at, split, reach, most):
    lead = EARLY[at] + OWN[at]
    out = [(0, EARLY[at])] * (EARLY[at] > 0) + [(EARLY[at], OWN[at])]
    return out + pieces(lead, split, 2) + pieces(split, reach, 2) + pieces(reach, most, 4)


def main_kernel(
    dims,
    sizes,
    scale,
    tab1,
    tab2,
    x_ref,
    out_ref,
    both1,
    both2,
    squares,
    zone1,
    zone2,
    outer1,
    outer2,
    pool,
    ahead,
    acc,
    isem,
    dsend,
    drecv,
    zs_sem,
    zr_sem,
    zf_send,
    zf_recv,
    xs_sem,
    xr_sem,
    ys_sem,
):
    rows, grid_c, slots = dims
    held = rows * slots
    half = zone_half(slots)
    lay = layout(rows, slots)
    grp, col = lax.axis_index("grp"), lax.axis_index("col")
    grps = lax.axis_size("grp")
    quad = lax.rem(col, 4)
    odd = lax.rem(col, 2)
    facing = (quad == 1) | (quad == 2)
    sign = 1 - 2 * odd
    partner = (grp, col + sign)
    above = (lax.rem(grp + 1, grps), col)
    below = (lax.rem(grp + grps - 1, grps), col)
    across = (grp, lax.rem(col - sign + grid_c, grid_c))
    relay = (grp, lax.rem(col - 3 * sign + grid_c, grid_c))

    loads = [
        pltpu.make_async_copy(x_ref, squares, isem.at[0]),
        pltpu.make_async_copy(x_ref, both1.at[pl.ds(0, held)], isem.at[1]),
    ]
    for load in loads:
        load.start()
    barrier = pltpu.get_barrier_semaphore()
    for peer in (partner, relay):
        pl.semaphore_signal(barrier, inc=1, device_id=peer, device_id_type=MESH)

    @pl.when(facing)
    def _():
        pl.semaphore_signal(barrier, inc=1, device_id=across, device_id_type=MESH)
        pl.semaphore_wait(barrier, 3)

    @pl.when(jnp.logical_not(facing))
    def _():
        for peer in (above, below):
            pl.semaphore_signal(barrier, inc=1, device_id=peer, device_id_type=MESH)
        pl.semaphore_wait(barrier, 4)

    def remote(src, dst, send_sem, recv_sem, peer):
        return pltpu.make_async_remote_copy(
            src_ref=src, dst_ref=dst, send_sem=send_sem, recv_sem=recv_sem, device_id=peer, device_id_type=MESH
        )

    def each(lo, hi, body):
        def one(i, carry):
            body(i)
            return carry

        lax.fori_loop(lo, hi, one, 0)

    def product(tab, row, a, right):
        code = tab[a, row]
        return jnp.dot(
            both1[lax.div(code, PACK)], right[lax.rem(code, PACK)], preferred_element_type=jnp.float32
        )

    def totals(tab, a, base, terms, wide, right, put):
        def one(i, carry):
            sums = [None] * wide
            for j in range(terms):
                for q in range(wide):
                    term = product(tab, base + j * 8 + i * wide + q, a, right)
                    sums[q] = term if sums[q] is None else sums[q] + term
            for q in range(wide):
                put(i * wide + q, sums[q])
            return carry

        lax.fori_loop(0, slots // wide, one, 0)

    def phase(at, tab, src, both, zone, outer, sizes, early_x, early_z, finish):
        split, reach, most, zn = sizes
        not_facing = jnp.logical_not(facing)
        spread = remote(src, both.at[pl.ds(held, held)], dsend.at[at], drecv.at[at], partner)
        spread.start()
        parts = cut(at, split, reach, most)
        n_lead = 1 + (EARLY[at] > 0)
        lead = EARLY[at] + OWN[at]
        xcopies, ycopies = [], []
        for i, (lo, n) in enumerate(parts):
            place = outer.at[pl.ds(lo, n)]
            held_at = ahead.at[pl.ds(0, n)] if i < n_lead - 1 else pool.at[pl.ds(lo, n)]
            xcopies.append(remote(held_at, place, xs_sem.at[at, i], xr_sem.at[at, i], across))
            passing = lead <= lo < reach
            ycopies.append(remote(place, place, ys_sem.at[at, i], xr_sem.at[at, i], relay) if passing else None)
        early = sum(lo < split for lo, _ in parts)
        passed = range(n_lead, sum(lo < reach for lo, _ in parts))
        zlead = ZEARLY[at] + ZOWN[at]
        zcopies, zpass = [[], []], []
        for s, peer in ((0, above), (1, below)):
            for i, (lo, n) in enumerate(((0, ZEARLY[at]), (ZEARLY[at], ZOWN[at]), (zlead, zn - zlead))):
                if n:
                    held_at = ahead.at[pl.ds(s * n, n)] if i == 0 else pool.at[pl.ds(s * half + lo, n)]
                    sems = zs_sem.at[at, s, i], zr_sem.at[at, s, i]
                    zcopies[s].append(remote(held_at, zone.at[pl.ds(s * half + lo, n)], *sems, peer))
            piece = pl.ds(s * half, zn)
            zpass.append(remote(zone.at[piece], zone.at[piece], zf_send.at[at, s], zf_recv.at[at, s], partner))

        def gather(dst, src, base, lo, n, to):
            def one(j):
                dst[to + j] = src[lax.max(tab[0, base + j] - 1, 0)]

            each(lo, lo + n, one)

        @pl.when(facing)
        def _():
            gather(pool, src, lay["pool"], EARLY[at], OWN[at], 0)
            xcopies[n_lead - 1].start()

        @pl.when(not_facing)
        def _():
            for s, base in ((0, lay["up"]), (1, lay["down"])):
                gather(pool, src, base, ZEARLY[at], ZOWN[at], s * half)
                zcopies[s][-2].start()

        if at == 0:
            loads[1].wait()
            both[2 * held] = jnp.zeros(both.shape[1:], both.dtype)
        spread.wait_recv()

        @pl.when(facing)
        def _():
            for i in range(n_lead, early):
                gather(pool, both, lay["pool"], *parts[i], 0)
                xcopies[i].start()

        @pl.when(not_facing)
        def _():
            for s, base in ((0, lay["up"]), (1, lay["down"])):
                gather(pool, both, base, zlead, zn - zlead, s * half)
                zcopies[s][-1].start()

        def inner(a):
            def put(f, total):
                acc[a * slots + f] = total

            totals(tab, a, 0, 6, 1, both, put)

        def pass_on(i):
            xcopies[i].wait_recv()
            ycopies[i].start()

        woven = min(rows, early - n_lead - 1)

        def weave(a):
            inner(a)

            @pl.when(facing & (a < woven))
            def _():
                place = outer.at[pl.ds(lead + 2 * a, 2)]
                sems = ys_sem.at[at, n_lead + a], xr_sem.at[at, n_lead + a]
                remote(pool.at[pl.ds(lead + 2 * a, 2)], place, xs_sem.at[at, n_lead + a], sems[1], across).wait_recv()
                remote(place, place, *sems, relay).start()

        each(0, rows, weave)

        @pl.when(facing)
        def _():
            for i in range(n_lead + woven, early - 1):
                pass_on(i)
            for copy in zpass:
                copy.wait_recv()

            def one(j):
                code = tab[0, lay["pool"] + j]
                far = (code > PACK).astype(jnp.int32)
                a = both[lax.max(code - 1, 0) * (1 - far)].astype(jnp.float32)
                b = zone[(code - PACK - 1) * far].astype(jnp.float32)
                w = far.astype(jnp.float32)
                pool[j] = (a * (1.0 - w) + b * w).astype(pool.dtype)

            for i in range(early, len(parts)):
                lo, n = parts[i]
                each(lo, lo + n, one)
                xcopies[i].start()
            early_x()

        @pl.when(not_facing)
        def _():
            early_z()
            for s in range(2):
                for copy in zcopies[s]:
                    copy.wait_recv()
                zpass[s].start()

        def edge(e):
            a = e * (rows - 1)

            def put(f, total):
                acc[a * slots + f] += total

            totals(tab, a, 48, 2, 1, zone, put)

        each(0, 2, edge)

        @pl.when(facing)
        def _():
            for i in passed:
                if i >= max(early - 1, n_lead + woven):
                    pass_on(i)
            for i in range(n_lead):
                xcopies[i].wait_recv()
            for i in range(passed.stop, len(parts)):
                xcopies[i].wait_recv()

        @pl.when(not_facing)
        def _():
            for i in passed:
                ycopies[i].wait_recv()

        def last(a):
            def put(f, total):
                finish(a, f, acc[a * slots + f] + total)

            totals(tab, a, 64, 3, 3 if slots % 3 == 0 else 1, outer, put)

        spread.wait_send()
        each(0, rows, last)

        @pl.when(facing)
        def _():
            for copy in xcopies + [ycopies[i] for i in passed]:
                copy.wait_send()

        @pl.when(not_facing)
        def _():
            for copy in zcopies[0] + zcopies[1] + zpass:
                copy.wait_send()

    def square(a, f, total):
        value = total.astype(squares.dtype)
        squares[a * slots + f] = value
        both2[a * slots + f] = value

    def step(a, f, total):
        used = tab1[a, lay["used"] + f].astype(jnp.float32)
        value = 1.5 * both1[a * slots + f].astype(jnp.float32) - total * scale
        out_ref[a * slots + f] = (value * used).astype(out_ref.dtype)

    def take(to, row, n):
        def one(j):
            ahead[to + j] = acc[lax.max(tab2[0, row + j] - 1, 0)].astype(ahead.dtype)

        each(0, n, one)

    def early_x():
        take(0, lay["pool"], EARLY[1])
        place = outer2.at[pl.ds(0, EARLY[1])]
        remote(ahead.at[pl.ds(0, EARLY[1])], place, xs_sem.at[1, 0], xr_sem.at[1, 0], across).start()

    def early_z():
        n = ZEARLY[1]
        for s, base, peer in ((0, lay["up"], above), (1, lay["down"], below)):
            take(s * n, base, n)
            place = zone2.at[pl.ds(s * half, n)]
            remote(ahead.at[pl.ds(s * n, n)], place, zs_sem.at[1, s, 0], zr_sem.at[1, s, 0], peer).start()

    loads[0].wait()
    phase(0, tab1, squares, both1, zone1, outer1, sizes[:4], early_x, early_z, square)
    nothing = lambda: None
    phase(1, tab2, squares, both2, zone2, outer2, sizes[4:], nothing, nothing, step)


def local(x_blocks, columns, filter_ids):
    grps, ncol = lax.axis_size("grp"), lax.axis_size("col")
    rows, per_col, slots, order = x_blocks.shape[:4]
    assert per_col == 1 and filter_ids.shape[2] == slots and ncol % 4 == 0 and rows > 1
    grid_a, grid_c = rows * grps, ncol
    count = grid_a * grid_c
    held = rows * slots
    blocks = x_blocks.reshape(held, order, order)
    dtype = blocks.dtype
    full = ()
    for n in EARLY:
        full += (2 * held + n, 2 * held + n + 4 * slots, 2 * held + n + 4 * slots, zone_half(slots))
    levels = [s for s in STAIRS if max(s[:3] + s[4:7]) < full[0]] + [full]
    lay = layout(rows, slots)
    vmem = pl.BlockSpec(memory_space=pltpu.VMEM)
    smem = pl.BlockSpec(memory_space=pltpu.SMEM)
    anyw = pl.BlockSpec(memory_space=pl.ANY)
    table = jax.ShapeDtypeStruct((8, lay["width"]), jnp.int32)
    tab1, tab2, level = pl.pallas_call(
        functools.partial(plan_kernel, (rows, grid_a, grid_c, slots, levels)),
        out_shape=[table, table, jax.ShapeDtypeStruct((1,), jnp.int32)],
        in_specs=[vmem, vmem],
        out_specs=[vmem, vmem, smem],
        scratch_shapes=[
            pltpu.VMEM((lay["end"] - lay["up"], count), jnp.int32),
            pltpu.VMEM((lay["width"], 128), jnp.int32),
        ],
        name="plan",
    )(columns.transpose(2, 1, 0), filter_ids.transpose(2, 1, 0))

    def blocks_of(n):
        return pltpu.VMEM((n, order, order), dtype)

    branches = []
    for i, sizes in enumerate(levels):
        most1, most2 = sizes[2], sizes[6]
        parts = max(len(cut(0, *sizes[:3])), len(cut(1, *sizes[4:7])))
        dma = pltpu.SemaphoreType.DMA
        branches.append(
            pl.pallas_call(
                functools.partial(main_kernel, (rows, grid_c, slots), sizes, 0.5 / (slots * order)),
                out_shape=pltpu.VMEM(blocks.shape, dtype),
                in_specs=[smem, smem, anyw],
                out_specs=vmem,
                scratch_shapes=[
                    blocks_of(2 * held + 1),
                    blocks_of(2 * held),
                    blocks_of(held),
                    blocks_of(2 * zone_half(slots)),
                    blocks_of(2 * zone_half(slots)),
                    blocks_of(most1),
                    blocks_of(most2),
                    blocks_of(max(most1, most2, 2 * zone_half(slots))),
                    blocks_of(max(EARLY[1], 2 * ZEARLY[1])),
                    pltpu.VMEM((held, order, order), jnp.float32),
                    dma((2,)),
                    dma((2,)),
                    dma((2,)),
                    dma((2, 2, 3)),
                    dma((2, 2, 3)),
                    dma((2, 2)),
                    dma((2, 2)),
                    dma((2, parts)),
                    dma((2, parts)),
                    dma((2, parts)),
                ],
                compiler_params=pltpu.CompilerParams(
                    collective_id=i, has_side_effects=True, vmem_limit_bytes=LIMIT
                ),
                name="step_%d_%d" % (most1, most2),
            )
        )
    out = lax.switch(level[0], branches, tab1, tab2, blocks)
    return out.reshape(x_blocks.shape)


def solution(mesh):
    return jax.shard_map(
        local,
        mesh=mesh,
        in_specs=(P("grp", "col", None, None, None), P(), P()),
        out_specs=P("grp", "col", None, None, None),
        check_vma=False,
    )
```
